128 devices in a mesh: row: 16 (over y, z_hi, core), col: 8 (over x, z_lo).
Axes of the slice: x: 4, y: 4, z: 4 (z_hi: 2, z_lo: 2; z = z_hi * 2 + z_lo), core: 2. Of those that a mesh axis runs over, the one named last changes fastest.
Arguments:
- homolog_embedding: bfloat16 [128, 1024, 64], P(('row', 'col')), may hold values from -6 to 6
- split_mapping_matrix: bfloat16 [64, 64], replicated, may hold values from -0.75 to 0.75
- couple_mapping_matrix: bfloat16 [1024, 128], replicated, may hold values from -1.5 to 1.5
- couple_offset_vector: bfloat16 [128], replicated, may hold values from -3 to 3
- incoming_adjoint_couple: bfloat16 [1024, 1024, 128], P('row', 'col'), may hold values from -0.29882812 to 0.29882812
Outputs:
- pair_delta_output: bfloat16 [1024, 1024, 128], P('row', 'col')
- alignment_gradient: bfloat16 [128, 1024, 64], P(('row', 'col'))
- out_weight_grad: float32 [1024, 128], replicated
The draws below stay inside these ranges and needn't reach their ends.
All inputs are finite; a program needn't handle non-finite values.
Results may differ from the reference program's by a relative error of at most 0.015.
Values may be sent and summed in bfloat16 or wider, within the bound.
A program may use at most 64 MiB of HBM per device.

```python
import jax
import jax.numpy as jnp
from jax import lax

FEATURE_DEPTH = 64
HIDDEN_WIDTH = 32
CZ = 128
CHAIN_LENGTH = 1024
ROW_TOTAL = 128


def level_of(key, extent, cuts, low, largest):
    gain, own = 1.0, jax.random.fold_in(key, 6)
    for dim, shards_of in cuts:
        heights = jnp.exp(jax.random.uniform(jax.random.fold_in(own, dim), (shards_of,), jnp.float32, low / len(cuts), largest / len(cuts)))
        gain = gain * jnp.repeat(heights, extent[dim] // shards_of).reshape([-1 if axis == dim else 1 for axis in range(len(extent))])
    return gain


def centred(own_key, shape, width, bound, split=(), kind=jnp.bfloat16):
    values = width * jax.random.normal(own_key, shape, jnp.float32)
    if split:
        values = values * level_of(own_key, shape, split, -0.22, 0.18)
    return jnp.clip(values, -bound, bound).astype(kind)


def setup_inputs(seed: int = 0) -> dict:
    seeds = jax.random.split(jax.random.key(seed), 6)
    return {
        "homolog_embedding": centred(seeds[0], (ROW_TOTAL, CHAIN_LENGTH, FEATURE_DEPTH), 1.0, 6.0, ((0, 128),)),
        "split_mapping_matrix": centred(seeds[1], (FEATURE_DEPTH, 2 * HIDDEN_WIDTH), FEATURE_DEPTH ** -0.5, 0.75),
        "couple_mapping_matrix": centred(seeds[2], (HIDDEN_WIDTH * HIDDEN_WIDTH, CZ), 0.25, 1.5),
        "couple_offset_vector": centred(seeds[3], (CZ,), 0.5, 3.0),
        "incoming_adjoint_couple": centred(seeds[4], (CHAIN_LENGTH, CHAIN_LENGTH, CZ), 0.05, 0.29882812, ((0, 16), (1, 8))),
    }


def standardize_features(homolog_embedding):
    mapped_halves = homolog_embedding.astype(jnp.float32)
    center = lax.optimization_barrier(jnp.mean(mapped_halves, axis=-1, keepdims=True))
    spread = lax.optimization_barrier(jnp.mean((mapped_halves - center) * (mapped_halves - center), axis=-1, keepdims=True))
    reciprocal_spread = lax.rsqrt(spread + 1e-05)
    return ((mapped_halves - center) * reciprocal_spread, reciprocal_spread)

def reference(homolog_embedding, split_mapping_matrix, couple_mapping_matrix, couple_offset_vector, incoming_adjoint_couple):
    standardized_activations, reciprocal_spread = standardize_features(homolog_embedding)
    normalized_input = standardized_activations.astype(jnp.bfloat16)
    factors = jnp.dot(normalized_input, split_mapping_matrix, preferred_element_type=jnp.float32).astype(jnp.bfloat16)
    left = factors[..., :HIDDEN_WIDTH]
    right = factors[..., HIDDEN_WIDTH:]
    block_rows = min(CHAIN_LENGTH, 64)
    count = CHAIN_LENGTH // block_rows
    left_blocks = left.reshape(ROW_TOTAL, count, block_rows, HIDDEN_WIDTH).transpose(1, 0, 2, 3)
    cot_blocks = incoming_adjoint_couple.reshape(count, block_rows, CHAIN_LENGTH, CZ)
    right_wide = right.astype(jnp.float32)

    def advance(carry, inputs):
        weight_sum, right_sum = carry
        left_block, cot_block = inputs
        left_wide = left_block.astype(jnp.float32)
        outer = jnp.einsum('sic,sje->ijce', left_wide, right_wide) / ROW_TOTAL
        flat = outer.astype(jnp.bfloat16).reshape(block_rows * CHAIN_LENGTH, HIDDEN_WIDTH * HIDDEN_WIDTH)
        update = (jnp.dot(flat, couple_mapping_matrix, preferred_element_type=jnp.float32) + couple_offset_vector.astype(jnp.float32)).astype(jnp.bfloat16)
        grad_rows = cot_block.reshape(block_rows * CHAIN_LENGTH, CZ)
        outer_grad = jnp.dot(grad_rows, couple_mapping_matrix.T, preferred_element_type=jnp.float32).astype(jnp.bfloat16)
        outer_grad = outer_grad.reshape(block_rows, CHAIN_LENGTH, HIDDEN_WIDTH, HIDDEN_WIDTH).astype(jnp.float32)
        weight_sum = weight_sum + jnp.dot(flat.T, grad_rows, preferred_element_type=jnp.float32)
        left_grad = jnp.einsum('ijce,sje->sic', outer_grad, right_wide) / ROW_TOTAL
        right_sum = right_sum + jnp.einsum('ijce,sic->sje', outer_grad, left_wide) / ROW_TOTAL
        return ((weight_sum, right_sum), (update.reshape(block_rows, CHAIN_LENGTH, CZ), left_grad))
    start = (jnp.zeros((HIDDEN_WIDTH * HIDDEN_WIDTH, CZ), jnp.float32), jnp.zeros((ROW_TOTAL, CHAIN_LENGTH, HIDDEN_WIDTH), jnp.float32))
    (factor_weight_gradient, right_grad), (updates, left_grads) = lax.scan(advance, start, (left_blocks, cot_blocks))
    pair_delta_output = updates.reshape(CHAIN_LENGTH, CHAIN_LENGTH, CZ)
    left_grad = left_grads.transpose(1, 0, 2, 3).reshape(ROW_TOTAL, CHAIN_LENGTH, HIDDEN_WIDTH)
    both = jnp.concatenate([left_grad.astype(jnp.bfloat16), right_grad.astype(jnp.bfloat16)], axis=-1)
    normalized_gradient = jnp.dot(both, split_mapping_matrix.T, preferred_element_type=jnp.float32)
    first_factor = lax.optimization_barrier(jnp.mean(normalized_gradient, axis=-1, keepdims=True))
    second_factor = lax.optimization_barrier(jnp.mean(normalized_gradient * standardized_activations, axis=-1, keepdims=True))
    alignment_gradient = (reciprocal_spread * (normalized_gradient - first_factor - standardized_activations * second_factor)).astype(jnp.bfloat16)
    return (pair_delta_output, alignment_gradient, factor_weight_gradient)
```

```python
import functools

import jax
import jax.numpy as jnp
from jax import lax
from jax.experimental import pallas as pl
from jax.experimental.pallas import tpu as pltpu
from jax.sharding import PartitionSpec as P

BF = jnp.bfloat16
F32 = jnp.float32
MESH = pl.DeviceIdType.MESH
NT = (((1,), (1,)), ((), ()))
DMA = pltpu.SemaphoreType.DMA


def dot(a, b):
    return jnp.dot(a, b, preferred_element_type=F32)


def dnt(a, b):
    return lax.dot_general(a, b, NT, preferred_element_type=F32)


def place():
    r, q = lax.axis_index("row"), lax.axis_index("col")
    y, zh, c = lax.div(r, 4), lax.rem(lax.div(r, 2), 2), lax.rem(r, 2)
    x, zl = lax.div(q, 2), lax.rem(q, 2)
    return r, q, y, zh, c, x, zl


def row_of(y, zh, c):
    return y * 4 + zh * 2 + c


def remote(src, dst, send, recv, to):
    return pltpu.make_async_remote_copy(
        src_ref=src, dst_ref=dst, send_sem=send, recv_sem=recv, device_id=to, device_id_type=MESH
    )


def greet(r, q):
    barrier = pltpu.get_barrier_semaphore()
    for d in range(1, 16):
        pl.semaphore_signal(barrier, inc=1, device_id=(lax.rem(r + d, 16), q), device_id_type=MESH)
    for d in range(1, 8):
        pl.semaphore_signal(barrier, inc=1, device_id=(r, lax.rem(q + d, 8)), device_id_type=MESH)


def greeted():
    pl.semaphore_wait(pltpu.get_barrier_semaphore(), 22)


def standardized(x_ref):
    x = x_ref[0].astype(F32)
    centred = x - jnp.mean(x, axis=-1, keepdims=True)
    rstd = lax.rsqrt(jnp.mean(centred * centred, axis=-1, keepdims=True) + 1e-5)
    return centred * rstd, rstd


def widened(ws, t):
    left = ws[:, :32]
    tiled = jnp.concatenate([left] * 4, axis=1)
    lane = lax.broadcasted_iota(jnp.int32, (64, 128), 1)
    return jnp.where(lane // 32 == t, tiled, 0.0).astype(BF)


def swapped(outer, inner):
    n = outer * inner
    to = lax.broadcasted_iota(jnp.int32, (n, n), 0)
    at = lax.broadcasted_iota(jnp.int32, (n, n), 1)
    return (at == (to % outer) * inner + to // outer).astype(F32).astype(BF)


def project(ws, xhat, xs, lsend, rsend):
    xs[...] = xhat
    for t in range(4):
        part = xs[pl.ds(t, 256, stride=4), :].astype(BF)
        term = dot(part, widened(ws, t))
        acc = term if t == 0 else acc + term
    lsend[...] = acc.astype(BF).reshape(16, 16, 128)
    right = ws.T[32:, :].astype(BF)
    for q in range(8):
        rsend[q] = dnt(right, xs[q * 128 : (q + 1) * 128, :].astype(BF)).astype(BF)


def scatter_start(r, q, lsend, rsend, l1, r1, sems):
    ls, lr, rs, rr = sems
    out = []
    for d in range(1, 16):
        to = lax.rem(r + d, 16)
        cp = remote(lsend.at[to], l1.at[r], ls.at[d], lr.at[r], (to, q))
        cp.start()
        out.append(cp)
    for d in range(1, 8):
        to = lax.rem(q + d, 8)
        cp = remote(rsend.at[to], r1.at[q], rs.at[d], rr.at[q], (r, to))
        cp.start()
        out.append(cp)
    return out


def wait_row(r, q, buf, recv, send):
    for d in range(1, 16):
        at = lax.rem(r + d, 16)
        remote(buf.at[at], buf.at[at], send.at[d], recv.at[at], (at, q)).wait_recv()


def wait_col(r, q, buf, recv, send):
    for d in range(1, 8):
        at = lax.rem(q + d, 8)
        remote(buf.at[at], buf.at[at], send.at[d], recv.at[at], (r, at)).wait_recv()


class Sends:
    def __init__(self, buf, send, recv):
        self.buf, self.send, self.recv, self.n, self.all = buf, send, recv, 0, []

    def start(self, slot, to):
        ref = self.buf.at[:, slot]
        cp = remote(ref, ref, self.send.at[self.n], self.recv.at[slot], to)
        self.n += 1
        cp.start()
        self.all.append(cp)

    def arrived(self, slot, source):
        ref = self.buf.at[:, slot]
        remote(ref, ref, self.send.at[0], self.recv.at[slot], source).wait_recv()


def spread_left(p, sends):
    r, q, y, zh, c, x, zl = p
    over = x * 2 + 1 - zl
    sends.start(q, (r, over))
    for d in (1, 3, 2):
        sends.start(q, (r, lax.rem(x + d, 4) * 2 + zl))

    def relay():
        sends.arrived(over, (r, over))
        for d in (1, 3, 2):
            sends.start(over, (r, lax.rem(x + d, 4) * 2 + zl))

    def rest():
        for d in (1, 3, 2):
            xd = lax.rem(x + d, 4)
            sends.arrived(xd * 2 + zl, (r, xd * 2 + zl))
            sends.arrived(xd * 2 + 1 - zl, (r, xd * 2 + zl))

    return relay, rest


def spread_right(p, sends):
    r, q, y, zh, c, x, zl = p
    over = row_of(y, 1 - zh, c)
    mate = row_of(y, zh, 1 - c)
    sends.start(r, (over, q))
    for d in (1, 3, 2):
        sends.start(r, (row_of(lax.rem(y + d, 4), zh, c), q))
    sends.start(r, (mate, q))

    def relay():
        sends.arrived(over, (over, q))
        for d in (1, 3, 2):
            sends.start(over, (row_of(lax.rem(y + d, 4), zh, c), q))
        sends.start(over, (mate, q))

    def rest():
        for zz in (zh, 1 - zh):
            for d in (1, 3, 2):
                yd = lax.rem(y + d, 4)
                slot = row_of(yd, zz, c)
                sends.arrived(slot, (row_of(yd, zh, c), q))
                sends.start(slot, (mate, q))
        for zz in (zh, 1 - zh):
            for d in range(4):
                sends.arrived(row_of(lax.rem(y + d, 4), zz, 1 - c), (mate, q))

    return relay, rest


def natural_left(l3, l4, lt):
    order = swapped(8, 16)
    for a in range(16):
        rows = dot(order, l3[a].reshape(128, 128)) * (1.0 / 128.0)
        l4[a] = rows.astype(BF)
        lt[a * 128 : (a + 1) * 128, :] = rows.T.astype(BF)


def forward_kernel(x, ws_ref, l4, lt, rn, xs, lsend, rsend, l1, r1, l3, r3, ls, lr, rs, rr, l2s, l2r, r2s, r2r):
    p = place()
    r, q = p[0], p[1]
    greet(r, q)
    ws = ws_ref[...].astype(F32)
    xhat, _ = standardized(x)
    project(ws, xhat, xs, lsend, rsend)
    l1[r] = lsend[r]
    r1[q] = rsend[q]
    greeted()
    out = scatter_start(r, q, lsend, rsend, l1, r1, (ls, lr, rs, rr))
    left_order, right_order = swapped(16, 16), swapped(8, 32)
    wait_col(r, q, r1, rr, rs)
    r3[:, r] = dot(right_order, r1[...].reshape(256, 128)).reshape(32, 8, 128).astype(BF)
    rsends = Sends(r3, r2s, r2r)
    rrelay, rrest = spread_right(p, rsends)
    wait_row(r, q, l1, lr, ls)
    l3[:, q] = dot(left_order, l1[...].reshape(256, 128)).astype(BF).reshape(16, 16, 128)
    lsends = Sends(l3, l2s, l2r)
    lrelay, lrest = spread_left(p, lsends)
    rrelay()
    lrelay()
    lrest()
    natural_left(l3, l4, lt)
    rrest()
    for e in range(32):
        rn[e] = r3[e].reshape(128, 128)
    for cp in out + rsends.all + lsends.all:
        cp.wait_send()


def grad_outer(cot, wr, G, unroll):
    @pl.loop(0, 32 // unroll)
    def _(step):
        for u in range(unroll):
            p = step * unroll + u
            o = dnt(wr[...], cot[pl.ds(2 * p, 2)].reshape(256, 128)).astype(BF)
            for h in range(2):
                G[:, pl.ds(pl.multiple_of((2 * p + h) * 32, 32), 32), :] = o[:, h * 128 : (h + 1) * 128].reshape(32, 32, 128)


def outer_product(lt, R, O, unroll):
    @pl.loop(0, 16 // unroll)
    def _(step):
        for u in range(unroll):
            p = step * unroll + u
            o = dot(lt[...], jnp.concatenate([R[2 * p], R[2 * p + 1]], axis=1)).astype(BF)
            O[2 * p] = o[:, :128]
            O[2 * p + 1] = o[:, 128:]


def left_gradient(G, R, put, M):
    @pl.loop(0, 2048 // M)
    def _(m):
        rows = pl.ds(pl.multiple_of(m * M, M), M)
        for p in range(16):
            g = jnp.concatenate([G[2 * p, rows, :], G[2 * p + 1, rows, :]], axis=1)
            term = dnt(g, jnp.concatenate([R[2 * p], R[2 * p + 1]], axis=1))
            acc = term if p == 0 else acc + term
        put(m, acc * (1.0 / 128.0))


def right_gradient(G, l4, put, unroll):
    @pl.loop(0, 16 // unroll)
    def _(step):
        for u in range(unroll):
            p = step * unroll + u
            for k in range(8):
                rows = slice(k * 256, (k + 1) * 256)
                g = jnp.concatenate([G[2 * p, rows, :], G[2 * p + 1, rows, :]], axis=1)
                term = dot(jnp.concatenate([l4[2 * k], l4[2 * k + 1]], axis=1), g)
                acc = term if k == 0 else acc + term
            put(2 * p, acc[:, :128])
            put(2 * p + 1, acc[:, 128:])


def weight_gradient(O, cot, put, E):
    @pl.loop(0, 32 // E)
    def _(m):
        for p in range(32):
            x = jnp.concatenate(
                [O[pl.ds(m * E, E), (2 * p + h) * 32 : (2 * p + h + 1) * 32, :].reshape(E * 32, 128) for h in range(2)], axis=1
            )
            term = dot(x, cot[2 * p : 2 * p + 2].reshape(256, 128))
            acc = term if p == 0 else acc + term
        put(m, acc)


def of_row(O, i):
    return O[:, pl.ds(pl.multiple_of(i * 32, 32), 32), :].reshape(1024, 128)


def pair_update(O, wt, bias, out, unroll):
    @pl.loop(0, 32 // unroll)
    def _(step):
        for u in range(unroll):
            p = step * unroll + u
            y = dot(wt[...], jnp.concatenate([of_row(O, 2 * p), of_row(O, 2 * p + 1)], axis=1))
            for h in range(2):
                out[2 * p + h] = (y[:, h * 128 : (h + 1) * 128].T + bias[...]).astype(BF)


def middle_kernel(l4, lt, rn, cot, wr, wt, bias, out, lg, rg, wg, O, G):
    order = swapped(16, 8)
    grad_outer(cot, wr, G, 8)

    def put_right(e, v):
        rg[e] = v.reshape(8, 2, 8, 128).astype(BF)

    right_gradient(G, l4, put_right, 8)

    def put_left(m, v):
        v = v.astype(BF)
        for k in range(4):
            lg[m * 4 + k] = dnt(order, v[k * 128 : (k + 1) * 128, :]).astype(BF)

    left_gradient(G, rn, put_left, 512)
    outer_product(lt, rn, O, 4)

    def put_weight(m, v):
        wg[pl.ds(m * 4, 4)] = v.astype(BF).reshape(4, 64, 128)

    weight_gradient(O, cot, put_weight, 8)
    pair_update(O, wt, bias, out, 8)


def to_row(p, src, dst, send, recv):
    r, q = p[0], p[1]
    out = []
    for d in range(1, 16):
        to = lax.rem(r + d, 16)
        cp = remote(src(to), dst.at[r], send.at[d], recv.at[r], (to, q))
        cp.start()
        out.append(cp)
    return out


def to_col(p, src, dst, send, recv):
    r, q = p[0], p[1]
    out = []
    for d in range(1, 8):
        to = lax.rem(q + d, 8)
        cp = remote(src(to), dst.at[q], send.at[d], recv.at[q], (r, to))
        cp.start()
        out.append(cp)
    return out


def summed(buf, n):
    acc = buf[0].astype(F32)
    for k in range(1, n):
        acc = acc + buf[k].astype(F32)
    return acc


def backward_kernel(
    x, ws_ref, lg, rg, wg, grad, wout,
    ns, rc, rcs, ry, rys, rz, r6, rin, lx, lxs, lz, l6, lin, wr_, ws_sum, wc, wall, wf,
    one_s, one_r, ys, yr, xs_, xr, lo_s, lo_r, ro_s, ro_r, w1s, w1r, w2s, w2r, w3s, w3r,
):
    p = place()
    r, q, y, zh, c, xx, zl = p
    greet(r, q)
    ws = ws_ref[...].astype(F32)
    xhat, rstd = standardized(x)
    greeted()
    sent = []
    mate = (row_of(y, zh, 1 - c), q)
    core = remote(rg.at[:, :, 1 - c], rc, one_s.at[0], one_r.at[0], mate)
    core.start()
    xcp = []
    for d in (1, 3, 2):
        to = lax.rem(xx + d, 4)
        cp = remote(lg.at[:, pl.ds(to * 32, 32), :], lx.at[d - 1], xs_.at[d - 1], xr.at[d - 1], (r, to * 2 + zl))
        cp.start()
        xcp.append(cp)
    sent += to_row(p, lambda to: wg.at[to], wr_, w1s, w1r)
    wr_[r] = wg[r]
    core.wait_recv()
    for e in range(32):
        rcs[e] = (rg[e, :, c].astype(F32) + rc[e].astype(F32)).astype(BF)
    ycp = []
    for d in (1, 3, 2):
        to = lax.rem(y + d, 4)
        cp = remote(rcs.at[:, pl.ds(to * 2, 2)], ry.at[d - 1], ys.at[d - 1], yr.at[d - 1], (row_of(to, zh, c), q))
        cp.start()
        ycp.append(cp)
    wait_row(r, q, wr_, w1r, w1s)
    ws_sum[...] = summed(wr_, 16).astype(BF)
    wc[q] = ws_sum[...]
    sent += to_col(p, lambda to: ws_sum, wc, w2s, w2r)
    for cp in xcp:
        cp.wait_recv()
    for a in range(16):
        own = lg[a, pl.ds(pl.multiple_of(xx * 32, 32), 32), :].astype(F32)
        for d in range(3):
            own = own + lx[d, a].astype(F32)
        lxs[a] = own.astype(BF).reshape(2, 16, 128)
    lzc = remote(lxs.at[:, 1 - zl], lz, one_s.at[1], one_r.at[1], (r, xx * 2 + 1 - zl))
    lzc.start()
    wait_col(r, q, wc, w2r, w2s)
    wall[r] = summed(wc, 8).astype(BF)
    sent += to_row(p, lambda to: wall.at[r], wall, w3s, w3r)
    lzc.wait_recv()
    five = (lxs[:, zl].astype(F32) + lz[...].astype(F32)).astype(BF)
    l6[...] = dot(swapped(16, 16), five.reshape(256, 128)).astype(BF).reshape(16, 16, 128)
    lin[r] = l6[r]
    sent += to_row(p, lambda to: l6.at[to], lin, lo_s, lo_r)
    for cp in ycp:
        cp.wait_recv()
    for e in range(32):
        own = rcs[e, pl.ds(y * 2, 2)].astype(F32)
        for d in range(3):
            own = own + ry[d, e].astype(F32)
        rys[e] = own.astype(BF)
    rzc = remote(rys.at[:, 1 - zh], rz, one_s.at[2], one_r.at[2], (row_of(y, 1 - zh, c), q))
    rzc.start()
    rzc.wait_recv()
    five = rys[:, zh].astype(F32) + rz[...].astype(F32)
    r6[...] = dot(swapped(32, 8), five.reshape(256, 128).astype(BF)).astype(BF).reshape(8, 32, 128)
    rin[q] = r6[q]
    sent += to_col(p, lambda to: r6.at[to], rin, ro_s, ro_r)
    wait_row(r, q, lin, lo_r, lo_s)
    flat = lin[...].reshape(256, 128)
    for t in range(4):
        ns[pl.ds(t, 256, stride=4), :] = dnt(flat, widened(ws, t))
    wait_row(r, q, wall, w3r, w3s)
    for k in range(16):
        wf[k * 64 : (k + 1) * 64, :] = wall[k].astype(F32)
    for k in range(32):
        wout[k * 32 : (k + 1) * 32, :] = wf[pl.ds(k, 32, stride=32), :]
    wait_col(r, q, rin, ro_r, ro_s)
    right = ws[:, 32:].astype(BF)
    for k in range(8):
        rows = slice(k * 128, (k + 1) * 128)
        ns[rows, :] = ns[rows, :] + dnt(rin[k].astype(F32).T.astype(BF), right)
    ng = ns[...]
    first = jnp.mean(ng, axis=-1, keepdims=True)
    second = jnp.mean(ng * xhat, axis=-1, keepdims=True)
    grad[0] = (rstd * (ng - first - xhat * second)).astype(BF)
    for cp in [core, lzc, rzc] + xcp + ycp + sent:
        cp.wait_send()


VM = pl.BlockSpec(memory_space=pltpu.VMEM)


def call(kernel, outs, n_in, scratch, name, ident=None):
    extra = {} if ident is None else {"collective_id": ident, "has_side_effects": True}
    return pl.pallas_call(
        kernel,
        out_shape=tuple(jax.ShapeDtypeStruct(s, t) for s, t in outs),
        in_specs=[VM] * n_in,
        out_specs=(VM,) * len(outs),
        scratch_shapes=scratch,
        compiler_params=pltpu.CompilerParams(vmem_limit_bytes=60 << 20, **extra),
        name=name,
    )


def on_device(x, ws, w, bias, cot):
    v = lambda *s: pltpu.VMEM(s, BF)
    f = lambda *s: pltpu.VMEM(s, F32)
    l4, lt, rn = call(
        forward_kernel,
        [((16, 128, 128), BF), ((2048, 128), BF), ((32, 128, 128), BF)],
        2,
        [f(1024, 64), v(16, 16, 128), v(8, 32, 128), v(16, 16, 128), v(8, 32, 128), v(16, 8, 16, 128), v(32, 16, 8, 128)]
        + [DMA((16,)), DMA((16,)), DMA((8,)), DMA((8,)), DMA((7,)), DMA((8,)), DMA((15,)), DMA((16,))],
        "forward",
        0,
    )(x, ws)
    wr = w.reshape(32, 32, 128).swapaxes(0, 1).reshape(1024, 128)
    wt = wr.T
    pair, lg, rg, wg = call(
        middle_kernel,
        [((64, 128, 128), BF), ((16, 128, 128), BF), ((32, 8, 2, 8, 128), BF), ((16, 64, 128), BF)],
        7,
        [v(32, 2048, 128), v(32, 2048, 128)],
        "middle",
    )(l4, lt, rn, cot, wr, wt, bias.astype(F32).reshape(1, 128))
    grad, wout = call(
        backward_kernel,
        [((1, 1024, 64), BF), ((1024, 128), F32)],
        5,
        [f(1024, 64), v(32, 8, 8, 128), v(32, 8, 8, 128), v(3, 32, 2, 8, 128), v(32, 2, 8, 128), v(32, 8, 128), v(8, 32, 128), v(8, 32, 128)]
        + [v(3, 16, 32, 128), v(16, 2, 16, 128), v(16, 16, 128), v(16, 16, 128), v(16, 16, 128)]
        + [v(16, 64, 128), v(64, 128), v(8, 64, 128), v(16, 64, 128), f(1024, 128)]
        + [DMA((3,)), DMA((3,)), DMA((3,)), DMA((3,)), DMA((3,)), DMA((3,))]
        + [DMA((16,)), DMA((16,)), DMA((8,)), DMA((8,)), DMA((16,)), DMA((16,)), DMA((8,)), DMA((8,)), DMA((16,)), DMA((16,))],
        "backward",
        1,
    )(x, ws, lg, rg, wg)
    return pair, grad, wout


def solution(mesh):
    placed = (P(("row", "col"), None, None), P(), P(), P(), P("row", "col", None))
    return jax.shard_map(
        on_device,
        mesh=mesh,
        in_specs=placed,
        out_specs=(P("row", "col", None), P(("row", "col"), None, None), P()),
        check_vma=False,
    )
```

```python
import functools

import jax
import jax.numpy as jnp
from jax import lax
from jax.experimental import pallas as pl
from jax.experimental.pallas import tpu as pltpu
from jax.sharding import PartitionSpec as P

BF = jnp.bfloat16
F32 = jnp.float32
MESH = pl.DeviceIdType.MESH
NT = (((1,), (1,)), ((), ()))
DMA = pltpu.SemaphoreType.DMA


def dot(a, b):
    return jnp.dot(a, b, preferred_element_type=F32)


def dnt(a, b):
    return lax.dot_general(a, b, NT, preferred_element_type=F32)


def place():
    r, q = lax.axis_index("row"), lax.axis_index("col")
    y, zh, c = lax.div(r, 4), lax.rem(lax.div(r, 2), 2), lax.rem(r, 2)
    x, zl = lax.div(q, 2), lax.rem(q, 2)
    return r, q, y, zh, c, x, zl


def row_of(y, zh, c):
    return y * 4 + zh * 2 + c


def remote(src, dst, send, recv, to):
    return pltpu.make_async_remote_copy(
        src_ref=src, dst_ref=dst, send_sem=send, recv_sem=recv, device_id=to, device_id_type=MESH
    )


def greet(r, q):
    barrier = pltpu.get_barrier_semaphore()
    for d in range(1, 16):
        pl.semaphore_signal(barrier, inc=1, device_id=(lax.rem(r + d, 16), q), device_id_type=MESH)
    for d in range(1, 8):
        pl.semaphore_signal(barrier, inc=1, device_id=(r, lax.rem(q + d, 8)), device_id_type=MESH)


def greeted():
    pl.semaphore_wait(pltpu.get_barrier_semaphore(), 22)


def standardized(x_ref):
    x = x_ref[...].astype(F32)
    centred = x - jnp.mean(x, axis=0, keepdims=True)
    rstd = lax.rsqrt(jnp.mean(centred * centred, axis=0, keepdims=True) + 1e-5)
    return centred * rstd, rstd


def widened(ws, t):
    left = ws[:, :32]
    tiled = jnp.concatenate([left] * 4, axis=1)
    lane = lax.broadcasted_iota(jnp.int32, (64, 128), 1)
    return jnp.where(lane // 32 == t, tiled, 0.0).astype(BF)


def swapped(outer, inner):
    n = outer * inner
    to = lax.broadcasted_iota(jnp.int32, (n, n), 0)
    at = lax.broadcasted_iota(jnp.int32, (n, n), 1)
    return (at == (to % outer) * inner + to // outer).astype(F32).astype(BF)


def project(ws, xt, xs, lsend, rsend):
    right = ws.T[32:, :].astype(BF)
    for q in range(8):
        cols = xt[:, q * 128 : (q + 1) * 128]
        xs[q * 128 : (q + 1) * 128, :] = cols.T
        rsend[q] = dot(right, cols.astype(BF)).astype(BF)
    for t in range(4):
        part = xs[pl.ds(t, 256, stride=4), :].astype(BF)
        term = dot(part, widened(ws, t))
        acc = term if t == 0 else acc + term
    lsend[...] = acc.astype(BF).reshape(16, 16, 128)


def scatter_start(r, q, lsend, rsend, l1, r1, sems):
    ls, lr, rs, rr = sems
    out = []
    for d in range(1, 16):
        to = lax.rem(r + d, 16)
        cp = remote(lsend.at[to], l1.at[r], ls.at[d], lr.at[r], (to, q))
        cp.start()
        out.append(cp)
    for d in range(1, 8):
        to = lax.rem(q + d, 8)
        cp = remote(rsend.at[to], r1.at[q], rs.at[d], rr.at[q], (r, to))
        cp.start()
        out.append(cp)
    return out


def wait_row(r, q, buf, recv, send):
    for d in range(1, 16):
        at = lax.rem(r + d, 16)
        remote(buf.at[at], buf.at[at], send.at[d], recv.at[at], (at, q)).wait_recv()


def wait_col(r, q, buf, recv, send):
    for d in range(1, 8):
        at = lax.rem(q + d, 8)
        remote(buf.at[at], buf.at[at], send.at[d], recv.at[at], (r, at)).wait_recv()


class Sends:
    def __init__(self, buf, send, recv):
        self.buf, self.send, self.recv, self.n, self.all = buf, send, recv, 0, []

    def start(self, slot, to):
        ref = self.buf.at[:, slot]
        cp = remote(ref, ref, self.send.at[self.n], self.recv.at[slot], to)
        self.n += 1
        cp.start()
        self.all.append(cp)

    def arrived(self, slot, source):
        ref = self.buf.at[:, slot]
        remote(ref, ref, self.send.at[0], self.recv.at[slot], source).wait_recv()


def spread_left(p, sends):
    r, q, y, zh, c, x, zl = p
    over = x * 2 + 1 - zl
    sends.start(q, (r, over))
    for d in (1, 3, 2):
        sends.start(q, (r, lax.rem(x + d, 4) * 2 + zl))

    def relay():
        sends.arrived(over, (r, over))
        for d in (1, 3, 2):
            sends.start(over, (r, lax.rem(x + d, 4) * 2 + zl))

    def rest():
        for d in (1, 3, 2):
            xd = lax.rem(x + d, 4)
            sends.arrived(xd * 2 + zl, (r, xd * 2 + zl))
            sends.arrived(xd * 2 + 1 - zl, (r, xd * 2 + zl))

    return relay, rest


def spread_right(p, sends):
    r, q, y, zh, c, x, zl = p
    over = row_of(y, 1 - zh, c)
    mate = row_of(y, zh, 1 - c)
    sends.start(r, (over, q))
    for d in (1, 3, 2):
        sends.start(r, (row_of(lax.rem(y + d, 4), zh, c), q))
    sends.start(r, (mate, q))

    def relay():
        sends.arrived(over, (over, q))
        for d in (1, 3, 2):
            sends.start(over, (row_of(lax.rem(y + d, 4), zh, c), q))
        sends.start(over, (mate, q))

    def pass_on():
        for zz in (zh, 1 - zh):
            for d in (1, 3, 2):
                yd = lax.rem(y + d, 4)
                slot = row_of(yd, zz, c)
                sends.arrived(slot, (row_of(yd, zh, c), q))
                sends.start(slot, (mate, q))

    def rest():
        for zz in (zh, 1 - zh):
            for d in range(4):
                sends.arrived(row_of(lax.rem(y + d, 4), zz, 1 - c), (mate, q))

    return relay, pass_on, rest


def natural_left(l3, l4, lt):
    order = swapped(8, 16)
    for a in range(16):
        rows = dot(order, l3[a].reshape(128, 128)) * (1.0 / 128.0)
        l4[a] = rows.astype(BF)
        lt[a * 128 : (a + 1) * 128, :] = rows.T.astype(BF)


def steps(lo, hi, body):
    if hi - lo == 1:
        body(lo)
    else:
        pl.loop(lo, hi)(body)


def grad_outer(cot, wr, G, lo, hi, unroll=8):
    def body(step):
        for u in range(unroll):
            p = step * unroll + u
            o = dnt(wr[...], cot[pl.ds(2 * p, 2)].reshape(256, 128)).astype(BF)
            for h in range(2):
                G[:, pl.ds(pl.multiple_of((2 * p + h) * 32, 32), 32), :] = o[:, h * 128 : (h + 1) * 128].reshape(32, 32, 128)

    steps(lo, hi, body)


def outer_product(lt, R, O, lo, hi, unroll=4):
    def body(step):
        for u in range(unroll):
            p = step * unroll + u
            o = dot(lt[...], jnp.concatenate([R[2 * p], R[2 * p + 1]], axis=1)).astype(BF)
            O[2 * p] = o[:, :128]
            O[2 * p + 1] = o[:, 128:]

    steps(lo, hi, body)


def left_gradient(G, R, put, lo, hi, M=512):
    def body(m):
        rows = pl.ds(pl.multiple_of(m * M, M), M)
        for p in range(16):
            g = jnp.concatenate([G[2 * p, rows, :], G[2 * p + 1, rows, :]], axis=1)
            term = dnt(g, jnp.concatenate([R[2 * p], R[2 * p + 1]], axis=1))
            acc = term if p == 0 else acc + term
        put(m, acc * (1.0 / 128.0))

    steps(lo, hi, body)


def right_gradient(G, l4, put, lo, hi, unroll=8):
    def body(step):
        for u in range(unroll):
            p = step * unroll + u
            for k in range(8):
                rows = slice(k * 256, (k + 1) * 256)
                g = jnp.concatenate([G[2 * p, rows, :], G[2 * p + 1, rows, :]], axis=1)
                term = dot(jnp.concatenate([l4[2 * k], l4[2 * k + 1]], axis=1), g)
                acc = term if k == 0 else acc + term
            put(2 * p, acc[:, :128])
            put(2 * p + 1, acc[:, 128:])

    steps(lo, hi, body)


def weight_gradient(O, cot, put, lo, hi, E=8):
    def body(m):
        for p in range(32):
            x = jnp.concatenate(
                [O[pl.ds(m * E, E), (2 * p + h) * 32 : (2 * p + h + 1) * 32, :].reshape(E * 32, 128) for h in range(2)], axis=1
            )
            term = dot(x, cot[2 * p : 2 * p + 2].reshape(256, 128))
            acc = term if p == 0 else acc + term
        put(m, acc)

    steps(lo, hi, body)


def of_row(O, i):
    return O[:, pl.ds(pl.multiple_of(i * 32, 32), 32), :].reshape(1024, 128)


def pair_update(O, wt, bias, out, lo, hi, unroll=8):
    wide = bias[...].astype(F32)

    def body(step):
        for u in range(unroll):
            p = step * unroll + u
            y = dot(wt[...], jnp.concatenate([of_row(O, 2 * p), of_row(O, 2 * p + 1)], axis=1))
            for h in range(2):
                out[2 * p + h] = (y[:, h * 128 : (h + 1) * 128].T + wide).astype(BF)

    steps(lo, hi, body)


def to_row(p, src, dst, send, recv):
    r, q = p[0], p[1]
    out = []
    for d in range(1, 16):
        to = lax.rem(r + d, 16)
        cp = remote(src(to), dst.at[r], send.at[d], recv.at[r], (to, q))
        cp.start()
        out.append(cp)
    return out


def to_col(p, src, dst, send, recv):
    r, q = p[0], p[1]
    out = []
    for d in range(1, 8):
        to = lax.rem(q + d, 8)
        cp = remote(src(to), dst.at[q], send.at[d], recv.at[q], (r, to))
        cp.start()
        out.append(cp)
    return out


def summed(buf, n):
    acc = buf[0].astype(F32)
    for k in range(1, n):
        acc = acc + buf[k].astype(F32)
    return acc


def whole_kernel(
    x, ws_ref, w, bias, cot_hbm, pair_hbm, grad, wout,
    xt, xs, wf, wr, wt, cot, pair, G, O,
    lsend, rsend, l1, r1, l3, r3, rn, l4, lt,
    rg, rc, rcs, ry, rys, rz, r6, rin, lg, lx, lxs, lz, l6, lin,
    wg, wgot, wsum, wc, wall,
    cot_sem, pair_sem,
    ls, lr, rs, rr, l2s, l2r, r2s, r2r,
    cs, cr, ys, yr, xs_s, xs_r, zs, zr, lo_s, lo_r, ro_s, ro_r, w1s, w1r, w2s, w2r, w3s, w3r,
):
    p = place()
    r, q, y, zh, c, xx, zl = p
    mate = (row_of(y, zh, 1 - c), q)
    greet(r, q)
    cot_copy = pltpu.make_async_copy(cot_hbm, cot, cot_sem.at[0])
    cot_copy.start()
    ws = ws_ref[...].astype(F32)
    xhat, rstd = standardized(x)
    xt[...] = xhat
    project(ws, xt, xs, lsend, rsend)
    l1[r] = lsend[r]
    r1[q] = rsend[q]
    greeted()
    sent = scatter_start(r, q, lsend, rsend, l1, r1, (ls, lr, rs, rr))
    wf[...] = w[...].astype(F32)
    for e in range(32):
        wr[e * 32 : (e + 1) * 32, :] = wf[pl.ds(e, 32, stride=32), :].astype(BF)
    for k in range(8):
        wt[:, k * 128 : (k + 1) * 128] = wr[k * 128 : (k + 1) * 128, :].astype(F32).T.astype(BF)
    left_order, right_order = swapped(16, 16), swapped(8, 32)
    cot_copy.wait()
    grad_outer(cot, wr, G, 0, 2)
    wait_col(r, q, r1, rr, rs)
    r3[:, r] = dot(right_order, r1[...].reshape(256, 128)).reshape(32, 8, 128).astype(BF)
    rsends = Sends(r3, r2s, r2r)
    rrelay, rpass, rrest = spread_right(p, rsends)
    wait_row(r, q, l1, lr, ls)
    l3[:, q] = dot(left_order, l1[...].reshape(256, 128)).astype(BF).reshape(16, 16, 128)
    lsends = Sends(l3, l2s, l2r)
    lrelay, lrest = spread_left(p, lsends)
    grad_outer(cot, wr, G, 2, 3)
    rrelay()
    lrelay()
    grad_outer(cot, wr, G, 3, 4)
    lrest()
    natural_left(l3, l4, lt)
    rpass()

    def put_right(e, v):
        rg[e] = v.reshape(8, 2, 8, 128).astype(BF)

    core = []
    for half in range(2):
        right_gradient(G, l4, put_right, half, half + 1)
        es = pl.ds(half * 16, 16)
        cp = remote(rg.at[es, :, 1 - c], rc.at[es], cs.at[half], cr.at[half], mate)
        cp.start()
        core.append(cp)
    rrest()
    for e in range(32):
        rn[e] = r3[e].reshape(128, 128)

    def put_weight(m, v):
        wg[m * 4 : (m + 1) * 4] = v.astype(BF).reshape(4, 64, 128)

    ycp = []
    for m in range(4):
        outer_product(lt, rn, O, m, m + 1)
        weight_gradient(O, cot, put_weight, m, m + 1)
        for k in range(4 * m, 4 * m + 4):
            @pl.when(r != k)
            def _():
                remote(wg.at[k], wgot.at[r], w1s.at[k], w1r.at[r], (k, q)).start()

        if m == 0:
            for cp in core:
                cp.wait_recv()
            for e in range(32):
                rcs[e] = (rg[e, :, c].astype(F32) + rc[e].astype(F32)).astype(BF)
            for d in (1, 3, 2):
                to = lax.rem(y + d, 4)
                cp = remote(rcs.at[:, pl.ds(to * 2, 2)], ry.at[d - 1], ys.at[d - 1], yr.at[d - 1], (row_of(to, zh, c), q))
                cp.start()
                ycp.append(cp)
    wgot[r] = wg[r]

    def put_left(m, v):
        v = v.astype(BF)
        for k in range(4):
            lg[m * 4 + k] = dnt(swapped(16, 8), v[k * 128 : (k + 1) * 128, :]).astype(BF)

    xcp = []
    one = []
    for m in range(4):
        left_gradient(G, rn, put_left, m, m + 1)
        rows = pl.ds(m * 4, 4)
        for d in (1, 3, 2):
            to = lax.rem(xx + d, 4)
            at = (d - 1) * 4 + m
            cp = remote(lg.at[rows, pl.ds(to * 32, 32), :], lx.at[d - 1, rows], xs_s.at[at], xs_r.at[at], (r, to * 2 + zl))
            cp.start()
            xcp.append(cp)
        if m == 0:
            for cp in ycp:
                cp.wait_recv()
            for e in range(32):
                own = rcs[e, pl.ds(y * 2, 2)].astype(F32)
                for d in range(3):
                    own = own + ry[d, e].astype(F32)
                rys[e] = own.astype(BF)
            rzc = remote(rys.at[:, 1 - zh], rz, zs.at[0], zr.at[0], (row_of(y, 1 - zh, c), q))
            rzc.start()
            one.append(rzc)
        if m == 1:
            wait_row(r, q, wgot, w1r, w1s)
            wsum[...] = summed(wgot, 16).astype(BF)
            wc[q] = wsum[...]
            sent += to_col(p, lambda to: wsum, wc, w2s, w2r)
        if m == 3:
            rzc.wait_recv()
            five = rys[:, zh].astype(F32) + rz[...].astype(F32)
            r6[...] = dot(swapped(32, 8), five.reshape(256, 128).astype(BF)).astype(BF).reshape(8, 32, 128)
            rin[q] = r6[q]
            sent += to_col(p, lambda to: r6.at[to], rin, ro_s, ro_r)
    wait_col(r, q, wc, w2r, w2s)
    wall[r] = summed(wc, 8).astype(BF)
    sent += to_row(p, lambda to: wall.at[r], wall, w3s, w3r)

    pcp = []
    for half in range(2):
        pair_update(O, wt, bias, pair, 2 * half, 2 * half + 2)
        rows = pl.ds(half * 32, 32)
        cp = pltpu.make_async_copy(pair.at[rows], pair_hbm.at[rows], pair_sem.at[half])
        cp.start()
        pcp.append(cp)
        if half == 0:
            for cp in xcp:
                cp.wait_recv()
            for a in range(16):
                own = lg[a, pl.ds(pl.multiple_of(xx * 32, 32), 32), :].astype(F32)
                for d in range(3):
                    own = own + lx[d, a].astype(F32)
                lxs[a] = own.astype(BF).reshape(2, 16, 128)
            lzc = remote(lxs.at[:, 1 - zl], lz, zs.at[1], zr.at[1], (r, xx * 2 + 1 - zl))
            lzc.start()
            one.append(lzc)
    lzc.wait_recv()
    five = (lxs[:, zl].astype(F32) + lz[...].astype(F32)).astype(BF)
    l6[...] = dot(swapped(16, 16), five.reshape(256, 128)).astype(BF).reshape(16, 16, 128)
    lin[r] = l6[r]
    sent += to_row(p, lambda to: l6.at[to], lin, lo_s, lo_r)
    wait_row(r, q, wall, w3r, w3s)
    for k in range(16):
        wf[k * 64 : (k + 1) * 64, :] = wall[k].astype(F32)
    for k in range(32):
        wout[k * 32 : (k + 1) * 32, :] = wf[pl.ds(k, 32, stride=32), :]
    wait_col(r, q, rin, ro_r, ro_s)
    wait_row(r, q, lin, lo_r, lo_s)
    flat = lin[...].reshape(256, 128)
    for t in range(4):
        xs[pl.ds(t, 256, stride=4), :] = dnt(flat, widened(ws, t))
    right = ws[:, 32:].astype(BF)
    for k in range(8):
        cols = slice(k * 128, (k + 1) * 128)
        ng = dot(right, rin[k]) + xs[cols, :].T
        xh = xt[:, cols]
        first = jnp.mean(ng, axis=0, keepdims=True)
        second = jnp.mean(ng * xh, axis=0, keepdims=True)
        grad[:, cols] = (rstd[:, cols] * (ng - first - xh * second)).astype(BF)
    for cp in sent + rsends.all + lsends.all + core + ycp + xcp + one:
        cp.wait_send()
    for k in range(16):
        @pl.when(r != k)
        def _():
            remote(wg.at[k], wgot.at[r], w1s.at[k], w1r.at[r], (k, q)).wait_send()

    for cp in pcp:
        cp.wait()


VM = pl.BlockSpec(memory_space=pltpu.VMEM)
ANY = pl.BlockSpec(memory_space=pl.ANY)


def on_device(x, ws, w, bias, cot):
    v = lambda *s: pltpu.VMEM(s, BF)
    f = lambda *s: pltpu.VMEM(s, F32)
    pair, grad, wout = pl.pallas_call(
        whole_kernel,
        out_shape=(
            jax.ShapeDtypeStruct((64, 128, 128), BF),
            jax.ShapeDtypeStruct((64, 1024), BF),
            jax.ShapeDtypeStruct((1024, 128), F32),
        ),
        in_specs=[VM, VM, VM, VM, ANY],
        out_specs=(ANY, VM, VM),
        scratch_shapes=[f(64, 1024), f(1024, 64), f(1024, 128), v(1024, 128), v(128, 1024), v(64, 128, 128), v(64, 128, 128)]
        + [v(32, 2048, 128), v(32, 2048, 128)]
        + [v(16, 16, 128), v(8, 32, 128), v(16, 16, 128), v(8, 32, 128), v(16, 8, 16, 128), v(32, 16, 8, 128), v(32, 128, 128)]
        + [v(16, 128, 128), v(2048, 128)]
        + [v(32, 8, 2, 8, 128), v(32, 8, 8, 128), v(32, 8, 8, 128), v(3, 32, 2, 8, 128), v(32, 2, 8, 128), v(32, 8, 128)]
        + [v(8, 32, 128), v(8, 32, 128)]
        + [v(16, 128, 128), v(3, 16, 32, 128), v(16, 2, 16, 128), v(16, 16, 128), v(16, 16, 128), v(16, 16, 128)]
        + [v(16, 64, 128), v(16, 64, 128), v(64, 128), v(8, 64, 128), v(16, 64, 128)]
        + [DMA((1,)), DMA((2,))]
        + [DMA((16,)), DMA((16,)), DMA((8,)), DMA((8,)), DMA((7,)), DMA((8,)), DMA((15,)), DMA((16,))]
        + [DMA((2,)), DMA((2,)), DMA((3,)), DMA((3,)), DMA((12,)), DMA((12,)), DMA((2,)), DMA((2,))]
        + [DMA((16,)), DMA((16,)), DMA((8,)), DMA((8,)), DMA((16,)), DMA((16,)), DMA((8,)), DMA((8,)), DMA((16,)), DMA((16,))],
        compiler_params=pltpu.CompilerParams(vmem_limit_bytes=60 << 20, collective_id=0, has_side_effects=True),
        name="whole",
    )(x[0].T, ws, w, bias.reshape(1, 128), cot)
    return pair, grad.T[None], wout


def solution(mesh):
    placed = (P(("row", "col"), None, None), P(), P(), P(), P("row", "col", None))
    return jax.shard_map(
        on_device,
        mesh=mesh,
        in_specs=placed,
        out_specs=(P("row", "col", None), P(("row", "col"), None, None), P()),
        check_vma=False,
    )
```

```python
import functools

import jax
import jax.numpy as jnp
from jax import lax
from jax.experimental import pallas as pl
from jax.experimental.pallas import tpu as pltpu
from jax.sharding import PartitionSpec as P

BF = jnp.bfloat16
F32 = jnp.float32
MESH = pl.DeviceIdType.MESH
NT = (((1,), (1,)), ((), ()))
DMA = pltpu.SemaphoreType.DMA


def dot(a, b):
    return jnp.dot(a, b, preferred_element_type=F32)


def dnt(a, b):
    return lax.dot_general(a, b, NT, preferred_element_type=F32)


def place():
    r, q = lax.axis_index("row"), lax.axis_index("col")
    y, zh, c = lax.div(r, 4), lax.rem(lax.div(r, 2), 2), lax.rem(r, 2)
    x, zl = lax.div(q, 2), lax.rem(q, 2)
    return r, q, y, zh, c, x, zl


def row_of(y, zh, c):
    return y * 4 + zh * 2 + c


def remote(src, dst, send, recv, to):
    return pltpu.make_async_remote_copy(
        src_ref=src, dst_ref=dst, send_sem=send, recv_sem=recv, device_id=to, device_id_type=MESH
    )


def greet(r, q):
    barrier = pltpu.get_barrier_semaphore()
    for d in range(1, 16):
        pl.semaphore_signal(barrier, inc=1, device_id=(lax.rem(r + d, 16), q), device_id_type=MESH)
    for d in range(1, 8):
        pl.semaphore_signal(barrier, inc=1, device_id=(r, lax.rem(q + d, 8)), device_id_type=MESH)


def greeted():
    pl.semaphore_wait(pltpu.get_barrier_semaphore(), 22)


def standardized(x_ref):
    x = x_ref[...].astype(F32)
    centred = x - jnp.mean(x, axis=0, keepdims=True)
    rstd = lax.rsqrt(jnp.mean(centred * centred, axis=0, keepdims=True) + 1e-5)
    return centred * rstd, rstd


def widened(ws, t):
    left = ws[:, :32]
    tiled = jnp.concatenate([left] * 4, axis=1)
    lane = lax.broadcasted_iota(jnp.int32, (64, 128), 1)
    return jnp.where(lane // 32 == t, tiled, 0.0).astype(BF)


def swapped(outer, inner):
    n = outer * inner
    to = lax.broadcasted_iota(jnp.int32, (n, n), 0)
    at = lax.broadcasted_iota(jnp.int32, (n, n), 1)
    return (at == (to % outer) * inner + to // outer).astype(F32).astype(BF)


def project(ws, xt, xs, lsend, rsend):
    right = ws.T[32:, :].astype(BF)
    for q in range(8):
        cols = xt[:, q * 128 : (q + 1) * 128]
        xs[q * 128 : (q + 1) * 128, :] = cols.T
        rsend[q] = dot(right, cols.astype(BF)).astype(BF)
    for t in range(4):
        part = xs[pl.ds(t, 256, stride=4), :].astype(BF)
        term = dot(part, widened(ws, t))
        acc = term if t == 0 else acc + term
    lsend[...] = acc.astype(BF).reshape(16, 16, 128)


def scatter_start(r, q, lsend, rsend, l1, r1, sems):
    ls, lr, rs, rr = sems
    out = []
    for d in range(1, 16):
        to = lax.rem(r + d, 16)
        cp = remote(lsend.at[to], l1.at[r], ls.at[d], lr.at[r], (to, q))
        cp.start()
        out.append(cp)
    for d in range(1, 8):
        to = lax.rem(q + d, 8)
        cp = remote(rsend.at[to], r1.at[q], rs.at[d], rr.at[q], (r, to))
        cp.start()
        out.append(cp)
    return out


def wait_row(r, q, buf, recv, send):
    for d in range(1, 16):
        at = lax.rem(r + d, 16)
        remote(buf.at[at], buf.at[at], send.at[d], recv.at[at], (at, q)).wait_recv()


def wait_col(r, q, buf, recv, send):
    for d in range(1, 8):
        at = lax.rem(q + d, 8)
        remote(buf.at[at], buf.at[at], send.at[d], recv.at[at], (r, at)).wait_recv()


class Sends:
    def __init__(self, buf, send, recv):
        self.buf, self.send, self.recv, self.n, self.all = buf, send, recv, 0, []

    def start(self, slot, to):
        ref = self.buf.at[:, slot]
        cp = remote(ref, ref, self.send.at[self.n], self.recv.at[slot], to)
        self.n += 1
        cp.start()
        self.all.append(cp)

    def arrived(self, slot, source):
        ref = self.buf.at[:, slot]
        remote(ref, ref, self.send.at[0], self.recv.at[slot], source).wait_recv()


def spread_left(p, sends):
    r, q, y, zh, c, x, zl = p
    over = x * 2 + 1 - zl
    sends.start(q, (r, over))
    for d in (1, 3, 2):
        sends.start(q, (r, lax.rem(x + d, 4) * 2 + zl))

    def relay():
        sends.arrived(over, (r, over))
        for d in (1, 3, 2):
            sends.start(over, (r, lax.rem(x + d, 4) * 2 + zl))

    def rest():
        for d in (1, 3, 2):
            xd = lax.rem(x + d, 4)
            sends.arrived(xd * 2 + zl, (r, xd * 2 + zl))
            sends.arrived(xd * 2 + 1 - zl, (r, xd * 2 + zl))

    return relay, rest


def spread_right(p, sends):
    r, q, y, zh, c, x, zl = p
    over = row_of(y, 1 - zh, c)
    mate = row_of(y, zh, 1 - c)
    sends.start(r, (over, q))
    for d in (1, 3, 2):
        sends.start(r, (row_of(lax.rem(y + d, 4), zh, c), q))
    sends.start(r, (mate, q))

    def relay():
        sends.arrived(over, (over, q))
        for d in (1, 3, 2):
            sends.start(over, (row_of(lax.rem(y + d, 4), zh, c), q))
        sends.start(over, (mate, q))

    def pass_on():
        for zz in (zh, 1 - zh):
            for d in (1, 3, 2):
                yd = lax.rem(y + d, 4)
                slot = row_of(yd, zz, c)
                sends.arrived(slot, (row_of(yd, zh, c), q))
                sends.start(slot, (mate, q))

    def rest():
        for zz in (zh, 1 - zh):
            for d in range(4):
                sends.arrived(row_of(lax.rem(y + d, 4), zz, 1 - c), (mate, q))

    return relay, pass_on, rest


def natural_left(l3, l4, lt):
    order = swapped(8, 16)
    for a in range(16):
        rows = dot(order, l3[a].reshape(128, 128)) * (1.0 / 128.0)
        l4[a] = rows.astype(BF)
        lt[a * 128 : (a + 1) * 128, :] = rows.T.astype(BF)


def steps(lo, hi, body):
    if hi - lo == 1:
        body(lo)
    else:
        pl.loop(lo, hi)(body)


def grad_outer(cot, wr, G, lo, hi, unroll=8):
    def body(step):
        for u in range(unroll):
            p = step * unroll + u
            o = dnt(wr[...], cot[pl.ds(2 * p, 2)].reshape(256, 128)).astype(BF)
            for h in range(2):
                G[:, pl.ds(pl.multiple_of((2 * p + h) * 32, 32), 32), :] = o[:, h * 128 : (h + 1) * 128].reshape(32, 32, 128)

    steps(lo, hi, body)


def outer_product(lt, R, O, at, m):
    for u in range(4):
        p = m * 4 + u
        o = dot(lt[...], jnp.concatenate([R[2 * p], R[2 * p + 1]], axis=1)).astype(BF)
        O[8 * at + 2 * u] = o[:, :128]
        O[8 * at + 2 * u + 1] = o[:, 128:]


def left_gradient(G, R, m, M=512):
    rows = slice(m * M, (m + 1) * M)
    for p in range(16):
        g = jnp.concatenate([G[2 * p, rows, :], G[2 * p + 1, rows, :]], axis=1)
        term = dnt(g, jnp.concatenate([R[2 * p], R[2 * p + 1]], axis=1))
        acc = term if p == 0 else acc + term
    return acc * (1.0 / 128.0)


def right_gradient(G, l4, put, lo, hi, unroll=8):
    def body(step):
        for u in range(unroll):
            p = step * unroll + u
            for k in range(8):
                rows = slice(k * 256, (k + 1) * 256)
                g = jnp.concatenate([G[2 * p, rows, :], G[2 * p + 1, rows, :]], axis=1)
                term = dot(jnp.concatenate([l4[2 * k], l4[2 * k + 1]], axis=1), g)
                acc = term if k == 0 else acc + term
            put(2 * p, acc[:, :128])
            put(2 * p + 1, acc[:, 128:])

    steps(lo, hi, body)


def weight_gradient(O, cot, at):
    for p in range(32):
        x = jnp.concatenate(
            [O[8 * at : 8 * at + 8, (2 * p + h) * 32 : (2 * p + h + 1) * 32, :].reshape(256, 128) for h in range(2)], axis=1
        )
        term = dot(x, cot[2 * p : 2 * p + 2].reshape(256, 128))
        acc = term if p == 0 else acc + term
    return acc


def of_row(O, i):
    return O[:, pl.ds(pl.multiple_of(i * 32, 32), 32), :].reshape(1024, 128)


def pair_update(O, wt, bias, out, lo, hi, unroll=8):
    wide = bias[...].astype(F32)

    def body(step):
        for u in range(unroll):
            p = step * unroll + u
            y = dot(wt[...], jnp.concatenate([of_row(O, 2 * p), of_row(O, 2 * p + 1)], axis=1))
            for h in range(2):
                out[2 * p + h] = (y[:, h * 128 : (h + 1) * 128].T + wide).astype(BF)

    steps(lo, hi, body)


def to_row(p, src, dst, send, recv):
    r, q = p[0], p[1]
    out = []
    for d in range(1, 16):
        to = lax.rem(r + d, 16)
        cp = remote(src(to), dst.at[r], send.at[d], recv.at[r], (to, q))
        cp.start()
        out.append(cp)
    return out


def to_col(p, src, dst, send, recv):
    r, q = p[0], p[1]
    out = []
    for d in range(1, 8):
        to = lax.rem(q + d, 8)
        cp = remote(src(to), dst.at[q], send.at[d], recv.at[q], (r, to))
        cp.start()
        out.append(cp)
    return out


def summed(buf, n):
    acc = buf[0].astype(F32)
    for k in range(1, n):
        acc = acc + buf[k].astype(F32)
    return acc


def whole_kernel(
    x, ws_ref, w, bias, cot_hbm, pair, grad, wall,
    xt, xs, wf, wr, wt, cot, G, O, raw, order,
    lsend, rsend, l1, r1, l3, r3, rn, l4, lt,
    rg, rc, rcs, ry, rys, rz, r6, rin, lg, lx, l6, lin,
    wg, wgot, wsum, wc,
    cot_sem,
    ls, lr, rs, rr, l2s, l2r, r2s, r2r,
    cs, cr, ys, yr, xs_s, xs_r, zs, zr, lo_s, lo_r, ro_s, ro_r, w1s, w1r, w2s, w2r, w3s, w3r,
):
    p = place()
    r, q, y, zh, c, xx, zl = p
    mate = (row_of(y, zh, 1 - c), q)
    greet(r, q)
    cot_copy = pltpu.make_async_copy(cot_hbm, cot, cot_sem.at[0])
    cot_copy.start()
    ws = ws_ref[...].astype(F32)
    xhat, rstd = standardized(x)
    xt[...] = xhat
    project(ws, xt, xs, lsend, rsend)
    l1[r] = lsend[r]
    r1[q] = rsend[q]
    greeted()
    sent = scatter_start(r, q, lsend, rsend, l1, r1, (ls, lr, rs, rr))
    wf[...] = w[...].astype(F32)
    for e in range(32):
        wr[e * 32 : (e + 1) * 32, :] = wf[pl.ds(e, 32, stride=32), :].astype(BF)
    chunk = [lax.rem(y + d, 4) for d in (2, 1, 3, 0)]
    for k in range(8):
        rows = pl.ds(pl.multiple_of(chunk[k // 2] * 256 + (k % 2) * 128, 128), 128)
        wt[:, k * 128 : (k + 1) * 128] = wr[rows, :].astype(F32).T.astype(BF)
    order[...] = swapped(16, 8)
    left_order, right_order = swapped(16, 16), swapped(8, 32)
    cot_copy.wait()
    grad_outer(cot, wr, G, 0, 2)
    wait_col(r, q, r1, rr, rs)
    r3[:, r] = dot(right_order, r1[...].reshape(256, 128)).reshape(32, 8, 128).astype(BF)
    rsends = Sends(r3, r2s, r2r)
    rrelay, rpass, rrest = spread_right(p, rsends)
    wait_row(r, q, l1, lr, ls)
    l3[:, q] = dot(left_order, l1[...].reshape(256, 128)).astype(BF).reshape(16, 16, 128)
    lsends = Sends(l3, l2s, l2r)
    lrelay, lrest = spread_left(p, lsends)
    grad_outer(cot, wr, G, 2, 3)
    rrelay()
    lrelay()
    grad_outer(cot, wr, G, 3, 4)
    lrest()
    natural_left(l3, l4, lt)
    rpass()

    def put_right(e, v):
        rg[e] = v.reshape(8, 2, 8, 128).astype(BF)

    core = []
    for half in range(2):
        right_gradient(G, l4, put_right, half, half + 1)
        es = pl.ds(half * 16, 16)
        cp = remote(rg.at[es, :, 1 - c], rc.at[es], cs.at[half], cr.at[half], mate)
        cp.start()
        core.append(cp)
    rrest()
    for e in range(32):
        rn[e] = r3[e].reshape(128, 128)

    ycp, xcp, one = [], [], []
    outer_product(lt, rn, O, 0, chunk[0])
    for at in range(4):
        if at < 3:
            outer_product(lt, rn, O, at + 1, chunk[at + 1])
        if at == 0:
            for cp in core:
                cp.wait_recv()
            for e in range(32):
                rcs[e] = (rg[e, :, c].astype(F32) + rc[e].astype(F32)).astype(BF)
            for d in (1, 3, 2):
                to = lax.rem(y + d, 4)
                cp = remote(rcs.at[:, pl.ds(to * 2, 2)], ry.at[d - 1], ys.at[d - 1], yr.at[d - 1], (row_of(to, zh, c), q))
                cp.start()
                ycp.append(cp)
        wg[4 * at : 4 * at + 4] = weight_gradient(O, cot, at).astype(BF).reshape(4, 64, 128)
        for k in range(4 if at < 3 else 3):
            piece = k if at < 3 else lax.rem(zh * 2 + c + k + 1, 4)
            sem = w1s.at[4 * at + k]
            cp = remote(wg.at[4 * at + piece], wgot.at[r], sem, w1r.at[r], (chunk[at] * 4 + piece, q))
            cp.start()
            sent.append(cp)
    wgot[r] = wg[12 + zh * 2 + c]

    def put_left(m):
        for k in range(4 * m, 4 * m + 4):
            lg[k] = dnt(order[...], raw[k * 128 : (k + 1) * 128, :]).astype(BF)
        rows = pl.ds(m * 4, 4)
        for d in (4, 5, 3, 6, 2, 7, 1):
            to = lax.rem(q + d, 8)
            at = (d - 1) * 4 + m
            src = lg.at[rows, pl.ds(pl.multiple_of(to * 16, 16), 16), :]
            cp = remote(src, lx.at[q, rows], xs_s.at[at], xs_r.at[q * 4 + m], (r, to))
            cp.start()
            sent.append(cp)

    for m in range(4):
        block = left_gradient(G, rn, m).astype(BF)
        if m > 0:
            put_left(m - 1)
        raw[m * 512 : (m + 1) * 512, :] = block
        if m == 0:
            for cp in ycp:
                cp.wait_recv()
            for e in range(32):
                own = rcs[e, pl.ds(y * 2, 2)].astype(F32)
                for d in range(3):
                    own = own + ry[d, e].astype(F32)
                rys[e] = own.astype(BF)
            rzc = remote(rys.at[:, 1 - zh], rz, zs.at[0], zr.at[0], (row_of(y, 1 - zh, c), q))
            rzc.start()
            one.append(rzc)
    put_left(3)
    wait_row(r, q, wgot, w1r, w1s)
    wsum[...] = summed(wgot, 16).astype(BF)
    wc[q] = wsum[...]
    sent += to_col(p, lambda to: wsum, wc, w2s, w2r)
    rzc.wait_recv()
    five = rys[:, zh].astype(F32) + rz[...].astype(F32)
    r6[...] = dot(swapped(32, 8), five.reshape(256, 128).astype(BF)).astype(BF).reshape(8, 32, 128)
    rin[q] = r6[q]
    sent += to_col(p, lambda to: r6.at[to], rin, ro_s, ro_r)
    order2 = swapped(16, 16)

    pair_update(O, wt, bias, pair, 0, 4)

    wait_col(r, q, wc, w2r, w2s)
    wall[r] = summed(wc, 8).astype(BF)
    sent += to_row(p, lambda to: wall.at[r], wall, w3s, w3r)
    for d in range(1, 8):
        at = lax.rem(q + d, 8)
        for m in range(4):
            ref = lx.at[at, pl.ds(m * 4, 4)]
            remote(ref, ref, xs_s.at[0], xs_r.at[at * 4 + m], (r, at)).wait_recv()
    lx[q] = lg[:, pl.ds(pl.multiple_of(q * 16, 16), 16), :]
    five = summed(lx, 8).astype(BF)
    l6[...] = dot(order2, five.reshape(256, 128)).astype(BF).reshape(16, 16, 128)
    lin[r] = l6[r]
    sent += to_row(p, lambda to: l6.at[to], lin, lo_s, lo_r)
    wait_row(r, q, wall, w3r, w3s)
    wait_col(r, q, rin, ro_r, ro_s)
    wait_row(r, q, lin, lo_r, lo_s)
    flat = lin[...].reshape(256, 128)
    for t in range(4):
        xs[pl.ds(t, 256, stride=4), :] = dnt(flat, widened(ws, t))
    right = ws[:, 32:].astype(BF)
    for k in range(8):
        cols = slice(k * 128, (k + 1) * 128)
        ng = dot(right, rin[k]) + xs[cols, :].T
        xh = xt[:, cols]
        first = jnp.mean(ng, axis=0, keepdims=True)
        second = jnp.mean(ng * xh, axis=0, keepdims=True)
        grad[:, cols] = (rstd[:, cols] * (ng - first - xh * second)).astype(BF)
    for cp in sent + rsends.all + lsends.all + core + ycp + xcp + one:
        cp.wait_send()


def finish_kernel(pair, grad, wall, pair_out, grad_out, wout, wf, sems):
    cps = [
        pltpu.make_async_copy(pair, pair_out, sems.at[0]),
        pltpu.make_async_copy(grad, grad_out, sems.at[1]),
    ]
    for cp in cps:
        cp.start()
    for k in range(16):
        wf[k * 64 : (k + 1) * 64, :] = wall[k].astype(F32)
    for k in range(32):
        wout[k * 32 : (k + 1) * 32, :] = wf[pl.ds(k, 32, stride=32), :]
    for cp in cps:
        cp.wait()


VM = pl.BlockSpec(memory_space=pltpu.VMEM)
ANY = pl.BlockSpec(memory_space=pl.ANY)


def on_device(x, ws, w, bias, cot):
    v = lambda *s: pltpu.VMEM(s, BF)
    f = lambda *s: pltpu.VMEM(s, F32)
    pair, grad, wall = pl.pallas_call(
        whole_kernel,
        out_shape=(v(64, 128, 128), v(64, 1024), v(16, 64, 128)),
        in_specs=[VM, VM, VM, VM, ANY],
        out_specs=(VM, VM, VM),
        scratch_shapes=[f(64, 1024), f(1024, 64), f(1024, 128), v(1024, 128), v(128, 1024), v(64, 128, 128)]
        + [v(32, 2048, 128), v(32, 2048, 128), v(2048, 128), v(128, 128)]
        + [v(16, 16, 128), v(8, 32, 128), v(16, 16, 128), v(8, 32, 128), v(16, 8, 16, 128), v(32, 16, 8, 128), v(32, 128, 128)]
        + [v(16, 128, 128), v(2048, 128)]
        + [v(32, 8, 2, 8, 128), v(32, 8, 8, 128), v(32, 8, 8, 128), v(3, 32, 2, 8, 128), v(32, 2, 8, 128), v(32, 8, 128)]
        + [v(8, 32, 128), v(8, 32, 128)]
        + [v(16, 128, 128), v(8, 16, 16, 128), v(16, 16, 128), v(16, 16, 128)]
        + [v(16, 64, 128), v(16, 64, 128), v(64, 128), v(8, 64, 128)]
        + [DMA((1,))]
        + [DMA((16,)), DMA((16,)), DMA((8,)), DMA((8,)), DMA((7,)), DMA((8,)), DMA((15,)), DMA((16,))]
        + [DMA((2,)), DMA((2,)), DMA((3,)), DMA((3,)), DMA((28,)), DMA((32,)), DMA((1,)), DMA((1,))]
        + [DMA((16,)), DMA((16,)), DMA((8,)), DMA((8,)), DMA((16,)), DMA((16,)), DMA((8,)), DMA((8,)), DMA((16,)), DMA((16,))],
        compiler_params=pltpu.CompilerParams(vmem_limit_bytes=54 << 20, collective_id=0, has_side_effects=True),
        name="whole",
    )(x[0].T, ws, w, bias.reshape(1, 128), cot)
    pair, grad, wout = pl.pallas_call(
        finish_kernel,
        out_shape=(
            jax.ShapeDtypeStruct((64, 128, 128), BF),
            jax.ShapeDtypeStruct((64, 1024), BF),
            jax.ShapeDtypeStruct((1024, 128), F32),
        ),
        in_specs=[VM, VM, VM],
        out_specs=(ANY, ANY, VM),
        scratch_shapes=[f(1024, 128), DMA((2,))],
        compiler_params=pltpu.CompilerParams(vmem_limit_bytes=8 << 20),
        name="finish",
    )(pair, grad, wall)
    return pair, grad.T[None], wout


def solution(mesh):
    placed = (P(("row", "col"), None, None), P(), P(), P(), P("row", "col", None))
    return jax.shard_map(
        on_device,
        mesh=mesh,
        in_specs=placed,
        out_specs=(P("row", "col", None), P(("row", "col"), None, None), P()),
        check_vma=False,
    )
```

```python
import functools

import jax
import jax.numpy as jnp
from jax import lax
from jax.experimental import pallas as pl
from jax.experimental.pallas import tpu as pltpu
from jax.sharding import PartitionSpec as P

BF = jnp.bfloat16
F32 = jnp.float32
MESH = pl.DeviceIdType.MESH
NT = (((1,), (1,)), ((), ()))
DMA = pltpu.SemaphoreType.DMA


def dot(a, b):
    return jnp.dot(a, b, preferred_element_type=F32)


def dnt(a, b):
    return lax.dot_general(a, b, NT, preferred_element_type=F32)


def place():
    r, q = lax.axis_index("row"), lax.axis_index("col")
    y, zh, c = lax.div(r, 4), lax.rem(lax.div(r, 2), 2), lax.rem(r, 2)
    x, zl = lax.div(q, 2), lax.rem(q, 2)
    return r, q, y, zh, c, x, zl


def row_of(y, zh, c):
    return y * 4 + zh * 2 + c


def remote(src, dst, send, recv, to):
    return pltpu.make_async_remote_copy(
        src_ref=src, dst_ref=dst, send_sem=send, recv_sem=recv, device_id=to, device_id_type=MESH
    )


def greet(r, q):
    barrier = pltpu.get_barrier_semaphore()
    for d in range(1, 16):
        pl.semaphore_signal(barrier, inc=1, device_id=(lax.rem(r + d, 16), q), device_id_type=MESH)
    for d in range(1, 8):
        pl.semaphore_signal(barrier, inc=1, device_id=(r, lax.rem(q + d, 8)), device_id_type=MESH)


def greeted():
    pl.semaphore_wait(pltpu.get_barrier_semaphore(), 22)


def standardized(x_ref):
    x = x_ref[...].astype(F32)
    centred = x - jnp.mean(x, axis=0, keepdims=True)
    rstd = lax.rsqrt(jnp.mean(centred * centred, axis=0, keepdims=True) + 1e-5)
    return centred * rstd, rstd


def widened(ws, t):
    left = ws[:, :32]
    tiled = jnp.concatenate([left] * 4, axis=1)
    lane = lax.broadcasted_iota(jnp.int32, (64, 128), 1)
    return jnp.where(lane // 32 == t, tiled, 0.0).astype(BF)


def swapped(outer, inner):
    n = outer * inner
    to = lax.broadcasted_iota(jnp.int32, (n, n), 0)
    at = lax.broadcasted_iota(jnp.int32, (n, n), 1)
    return (at == (to % outer) * inner + to // outer).astype(F32).astype(BF)


def project(ws, xt, xs, lsend, rsend):
    right = ws.T[32:, :].astype(BF)
    for q in range(8):
        cols = xt[:, q * 128 : (q + 1) * 128]
        xs[q * 128 : (q + 1) * 128, :] = cols.T
        rsend[q] = dot(right, cols.astype(BF)).astype(BF)
    for t in range(4):
        part = xs[pl.ds(t, 256, stride=4), :].astype(BF)
        term = dot(part, widened(ws, t))
        acc = term if t == 0 else acc + term
    lsend[...] = acc.astype(BF).reshape(16, 16, 128)


def taken(ref, sem, peer):
    remote(ref, ref, sem, sem, peer).wait_recv()


def gone(ref, sem, peer):
    remote(ref, ref, sem, sem, peer).wait_send()


def to_row(p, src, dst, sems):
    r, q = p[0], p[1]
    for d in range(1, 16):
        to = lax.rem(r + d, 16)
        remote(src(to), dst.at[r], sems.at[0], sems.at[1], (to, q)).start()


def to_col(p, src, dst, sems):
    r, q = p[0], p[1]
    for d in range(1, 8):
        to = lax.rem(q + d, 8)
        remote(src(to), dst.at[q], sems.at[0], sems.at[1], (r, to)).start()


class Sends:
    def __init__(self, buf, send, recv):
        self.buf, self.send, self.recv = buf, send, recv

    def start(self, slot, to, at):
        ref = self.buf.at[:, slot]
        remote(ref, ref, self.send.at[0], self.recv.at[at], to).start()

    def arrived(self, slot, source, at):
        taken(self.buf.at[:, slot], self.recv.at[at], source)


def spread_left(p, sends):
    r, q, y, zh, c, x, zl = p
    over = x * 2 + 1 - zl
    sends.start(q, (r, over), 0)
    for d in (1, 3, 2):
        sends.start(q, (r, lax.rem(x + d, 4) * 2 + zl), 1)

    def relay():
        sends.arrived(over, (r, over), 0)
        for d in (1, 3, 2):
            sends.start(over, (r, lax.rem(x + d, 4) * 2 + zl), 1)

    def rest():
        taken(sends.buf.at[:, pl.ds(0, 6)], sends.recv.at[1], (r, over))

    def left():
        gone(sends.buf.at[:, pl.ds(0, 7)], sends.send.at[0], (r, over))

    return relay, rest, left


def spread_right(p, sends):
    r, q, y, zh, c, x, zl = p
    over = row_of(y, 1 - zh, c)
    mate = row_of(y, zh, 1 - c)
    sends.start(r, (over, q), 0)
    for d in (1, 3, 2):
        sends.start(r, (row_of(lax.rem(y + d, 4), zh, c), q), d)
    sends.start(r, (mate, q), 7)

    def relay():
        sends.arrived(over, (over, q), 0)
        for d in (1, 3, 2):
            sends.start(over, (row_of(lax.rem(y + d, 4), zh, c), q), 3 + d)
        sends.start(over, (mate, q), 7)

    def pass_on():
        for far in range(2):
            zz = zh if far == 0 else 1 - zh
            for d in (3, 1, 2):
                yd = lax.rem(y + d, 4)
                slot = row_of(yd, zz, c)
                sends.arrived(slot, (row_of(yd, zh, c), q), 3 * far + 4 - d)
                sends.start(slot, (mate, q), 7)

    def rest():
        taken(sends.buf.at[:, pl.ds(0, 8)], sends.recv.at[7], (mate, q))

    def left():
        gone(sends.buf.at[:, pl.ds(0, 15)], sends.send.at[0], (mate, q))

    return relay, pass_on, rest, left


def natural_left(l3, l4, lt):
    order = swapped(8, 16)
    for a in range(16):
        rows = dot(order, l3[a].reshape(128, 128)) * (1.0 / 128.0)
        l4[a] = rows.astype(BF)
        lt[a * 128 : (a + 1) * 128, :] = rows.T.astype(BF)


def steps(lo, hi, body):
    if hi - lo == 1:
        body(lo)
    else:
        pl.loop(lo, hi)(body)


def grad_outer(cot, wr, G, lo, hi, unroll=8):
    def body(step):
        for u in range(unroll):
            p = step * unroll + u
            o = dnt(wr[...], cot[pl.ds(2 * p, 2)].reshape(256, 128)).astype(BF)
            for h in range(2):
                G[:, pl.ds(pl.multiple_of((2 * p + h) * 32, 32), 32), :] = o[:, h * 128 : (h + 1) * 128].reshape(32, 32, 128)

    steps(lo, hi, body)


def outer_product(lt, R, O, at, m):
    for u in range(4):
        p = m * 4 + u
        o = dot(lt[...], jnp.concatenate([R[2 * p], R[2 * p + 1]], axis=1)).astype(BF)
        O[8 * at + 2 * u] = o[:, :128]
        O[8 * at + 2 * u + 1] = o[:, 128:]


def left_gradient(G, R, m, M=512):
    rows = slice(m * M, (m + 1) * M)
    for p in range(16):
        g = jnp.concatenate([G[2 * p, rows, :], G[2 * p + 1, rows, :]], axis=1)
        term = dnt(g, jnp.concatenate([R[2 * p], R[2 * p + 1]], axis=1))
        acc = term if p == 0 else acc + term
    return acc * (1.0 / 128.0)


def right_gradient(G, l4, put, lo, hi, unroll=8):
    def body(step):
        for u in range(unroll):
            p = step * unroll + u
            for k in range(8):
                rows = slice(k * 256, (k + 1) * 256)
                g = jnp.concatenate([G[2 * p, rows, :], G[2 * p + 1, rows, :]], axis=1)
                term = dot(jnp.concatenate([l4[2 * k], l4[2 * k + 1]], axis=1), g)
                acc = term if k == 0 else acc + term
            put(2 * p, acc[:, :128])
            put(2 * p + 1, acc[:, 128:])

    steps(lo, hi, body)


def weight_gradient(O, cot, at):
    for p in range(32):
        x = jnp.concatenate(
            [O[8 * at : 8 * at + 8, (2 * p + h) * 32 : (2 * p + h + 1) * 32, :].reshape(256, 128) for h in range(2)], axis=1
        )
        term = dot(x, cot[2 * p : 2 * p + 2].reshape(256, 128))
        acc = term if p == 0 else acc + term
    return acc


def of_row(O, i):
    return O[:, pl.ds(pl.multiple_of(i * 32, 32), 32), :].reshape(1024, 128)


def pair_update(O, wt, bias, out, lo, hi, unroll=8):
    wide = bias[...].astype(F32)

    def body(step):
        for u in range(unroll):
            p = step * unroll + u
            y = dot(wt[...], jnp.concatenate([of_row(O, 2 * p), of_row(O, 2 * p + 1)], axis=1))
            for h in range(2):
                out[2 * p + h] = (y[:, h * 128 : (h + 1) * 128].T + wide).astype(BF)

    steps(lo, hi, body)


def summed(buf, n):
    acc = buf[0].astype(F32)
    for k in range(1, n):
        acc = acc + buf[k].astype(F32)
    return acc


def whole_kernel(
    x, ws_ref, w, bias, cot_hbm, pair, grad, wall,
    xt, ns, xs, wf, wr, wt, cot, G, O, raw, order,
    lsend, rsend, l1, r1, l3, r3, rn, l4, lt,
    rg, rc, rcs, ry, rys, rz, r6, rin, lg, lx, l6, lin,
    wg, wgot, wsum, wc,
    cot_sem,
    la, ra, l2s, l2r, r2s, r2r, cores, ys, lxsem, zs, lo, ro, w1, w2, w3,
):
    p = place()
    r, q, y, zh, c, xx, zl = p
    mate = (row_of(y, zh, 1 - c), q)
    beside = (r, lax.rem(q + 1, 8))
    greet(r, q)
    cot_copy = pltpu.make_async_copy(cot_hbm, cot, cot_sem.at[0])
    cot_copy.start()
    ws = ws_ref[...].astype(F32)
    xhat, rstd = standardized(x)
    xt[...] = xhat
    project(ws, xt, xs, lsend, rsend)
    l1[r] = lsend[r]
    r1[q] = rsend[q]
    greeted()
    to_col(p, lambda to: rsend.at[to], r1, ra)
    to_row(p, lambda to: lsend.at[to], l1, la)
    wf[...] = w[...].astype(F32)
    for e in range(32):
        wr[e * 32 : (e + 1) * 32, :] = wf[pl.ds(e, 32, stride=32), :].astype(BF)
    chunk = [lax.rem(y + d, 4) for d in (2, 1, 3, 0)]
    for k in range(8):
        rows = pl.ds(pl.multiple_of(chunk[k // 2] * 256 + (k % 2) * 128, 128), 128)
        wt[:, k * 128 : (k + 1) * 128] = wr[rows, :].astype(F32).T.astype(BF)
    order[...] = swapped(16, 8)
    left_order, right_order = swapped(16, 16), swapped(8, 32)
    cot_copy.wait()
    grad_outer(cot, wr, G, 0, 2)
    taken(r1.at[pl.ds(0, 7)], ra.at[1], beside)
    r3[:, r] = dot(right_order, r1[...].reshape(256, 128)).reshape(32, 8, 128).astype(BF)
    rsends = Sends(r3, r2s, r2r)
    rrelay, rpass, rrest, rleft = spread_right(p, rsends)
    taken(l1.at[pl.ds(0, 15)], la.at[1], mate)
    l3[:, q] = dot(left_order, l1[...].reshape(256, 128)).astype(BF).reshape(16, 16, 128)
    lsends = Sends(l3, l2s, l2r)
    lrelay, lrest, lleft = spread_left(p, lsends)
    grad_outer(cot, wr, G, 2, 3)
    rrelay()
    lrelay()
    grad_outer(cot, wr, G, 3, 4)
    lrest()
    natural_left(l3, l4, lt)
    rpass()

    def put_right(e, v):
        rg[e] = v.reshape(8, 2, 8, 128).astype(BF)

    for half in range(2):
        right_gradient(G, l4, put_right, half, half + 1)
        es = pl.ds(half * 16, 16)
        remote(rg.at[es, :, 1 - c], rc.at[es], cores.at[0], cores.at[1], mate).start()
    rrest()
    for e in range(32):
        rn[e] = r3[e].reshape(128, 128)

    outer_product(lt, rn, O, 0, chunk[0])
    for at in range(4):
        if at < 3:
            outer_product(lt, rn, O, at + 1, chunk[at + 1])
        if at == 0:
            taken(rc, cores.at[1], mate)
            for e in range(32):
                rcs[e] = (rg[e, :, c].astype(F32) + rc[e].astype(F32)).astype(BF)
            for d in (1, 3, 2):
                to = lax.rem(y + d, 4)
                remote(rcs.at[:, pl.ds(to * 2, 2)], ry.at[d - 1], ys.at[0], ys.at[1], (row_of(to, zh, c), q)).start()
        wg[4 * at : 4 * at + 4] = weight_gradient(O, cot, at).astype(BF).reshape(4, 64, 128)
        for k in range(4 if at < 3 else 3):
            piece = k if at < 3 else lax.rem(zh * 2 + c + k + 1, 4)
            remote(wg.at[4 * at + piece], wgot.at[r], w1.at[0], w1.at[1], (chunk[at] * 4 + piece, q)).start()
    wgot[r] = wg[12 + zh * 2 + c]

    def put_left(m):
        for k in range(4 * m, 4 * m + 4):
            lg[k] = dnt(order[...], raw[k * 128 : (k + 1) * 128, :]).astype(BF)
        rows = pl.ds(m * 4, 4)
        for d in (4, 5, 3, 6, 2, 7, 1):
            to = lax.rem(q + d, 8)
            src = lg.at[rows, pl.ds(pl.multiple_of(to * 16, 16), 16), :]
            remote(src, lx.at[q, rows], lxsem.at[0], lxsem.at[1], (r, to)).start()

    for m in range(4):
        block = left_gradient(G, rn, m).astype(BF)
        if m > 0:
            put_left(m - 1)
        raw[m * 512 : (m + 1) * 512, :] = block
        if m == 0:
            taken(ry, ys.at[1], mate)
            for e in range(32):
                own = rcs[e, pl.ds(y * 2, 2)].astype(F32)
                for d in range(3):
                    own = own + ry[d, e].astype(F32)
                rys[e] = own.astype(BF)
            rzc = remote(rys.at[:, 1 - zh], rz, zs.at[0], zs.at[1], (row_of(y, 1 - zh, c), q))
            rzc.start()
        if m == 2:
            taken(wgot.at[pl.ds(0, 15)], w1.at[1], mate)
            wsum[...] = summed(wgot, 16).astype(BF)
            wc[q] = wsum[...]
            to_col(p, lambda to: wsum, wc, w2)
    put_left(3)
    rzc.wait_recv()
    five = rys[:, zh].astype(F32) + rz[...].astype(F32)
    r6[...] = dot(swapped(32, 8), five.reshape(256, 128).astype(BF)).astype(BF).reshape(8, 32, 128)
    rin[q] = r6[q]
    to_col(p, lambda to: r6.at[to], rin, ro)
    order2 = swapped(16, 16)

    pair_update(O, wt, bias, pair, 0, 4)

    taken(wc.at[pl.ds(0, 7)], w2.at[1], beside)
    wall[r] = summed(wc, 8).astype(BF)
    to_row(p, lambda to: wall.at[r], wall, w3)
    taken(lx.at[pl.ds(0, 7)], lxsem.at[1], beside)
    lx[q] = lg[:, pl.ds(pl.multiple_of(q * 16, 16), 16), :]
    five = summed(lx, 8).astype(BF)
    l6[...] = dot(order2, five.reshape(256, 128)).astype(BF).reshape(16, 16, 128)
    lin[r] = l6[r]
    to_row(p, lambda to: l6.at[to], lin, lo)
    gone(rsend.at[pl.ds(0, 7)], ra.at[0], beside)
    gone(lsend.at[pl.ds(0, 15)], la.at[0], mate)
    rleft()
    lleft()
    gone(rc, cores.at[0], mate)
    gone(ry, ys.at[0], mate)
    rzc.wait_send()
    gone(wgot.at[pl.ds(0, 15)], w1.at[0], mate)
    gone(lx.at[pl.ds(0, 7)], lxsem.at[0], beside)
    gone(wc.at[pl.ds(0, 7)], w2.at[0], beside)
    gone(rin.at[pl.ds(0, 7)], ro.at[0], beside)
    taken(rin.at[pl.ds(0, 7)], ro.at[1], beside)
    right = ws[:, 32:].astype(BF)
    for k in range(8):
        ns[:, k * 128 : (k + 1) * 128] = dot(right, rin[k])
    taken(lin.at[pl.ds(0, 15)], lo.at[1], mate)
    flat = lin[...].reshape(256, 128)
    for t in range(4):
        xs[pl.ds(t, 256, stride=4), :] = dnt(flat, widened(ws, t))
    for k in range(8):
        cols = slice(k * 128, (k + 1) * 128)
        ng = ns[:, cols] + xs[cols, :].T
        xh = xt[:, cols]
        first = jnp.mean(ng, axis=0, keepdims=True)
        second = jnp.mean(ng * xh, axis=0, keepdims=True)
        grad[:, cols] = (rstd[:, cols] * (ng - first - xh * second)).astype(BF)
    taken(wall.at[pl.ds(0, 15)], w3.at[1], mate)
    gone(lin.at[pl.ds(0, 15)], lo.at[0], mate)
    gone(wall.at[pl.ds(0, 15)], w3.at[0], mate)


def finish_kernel(pair, grad, wall, pair_out, grad_out, wout, wf, wo, sems):
    cps = [
        pltpu.make_async_copy(pair, pair_out, sems.at[0]),
        pltpu.make_async_copy(grad, grad_out, sems.at[1]),
        pltpu.make_async_copy(wo, wout, sems.at[2]),
    ]
    cps[0].start()
    cps[1].start()
    for k in range(16):
        wf[k * 64 : (k + 1) * 64, :] = wall[k].astype(F32)
    for k in range(32):
        wo[k * 32 : (k + 1) * 32, :] = wf[pl.ds(k, 32, stride=32), :]
    cps[2].start()
    for cp in cps:
        cp.wait()


VM = pl.BlockSpec(memory_space=pltpu.VMEM)
ANY = pl.BlockSpec(memory_space=pl.ANY)


def on_device(x, ws, w, bias, cot):
    v = lambda *s: pltpu.VMEM(s, BF)
    f = lambda *s: pltpu.VMEM(s, F32)
    pair, grad, wall = pl.pallas_call(
        whole_kernel,
        out_shape=(v(64, 128, 128), v(64, 1024), v(16, 64, 128)),
        in_specs=[VM, VM, VM, VM, ANY],
        out_specs=(VM, VM, VM),
        scratch_shapes=[f(64, 1024), f(64, 1024), f(1024, 64), f(1024, 128), v(1024, 128), v(128, 1024), v(64, 128, 128)]
        + [v(32, 2048, 128), v(32, 2048, 128), v(2048, 128), v(128, 128)]
        + [v(16, 16, 128), v(8, 32, 128), v(16, 16, 128), v(8, 32, 128), v(16, 8, 16, 128), v(32, 16, 8, 128), v(32, 128, 128)]
        + [v(16, 128, 128), v(2048, 128)]
        + [v(32, 8, 2, 8, 128), v(32, 8, 8, 128), v(32, 8, 8, 128), v(3, 32, 2, 8, 128), v(32, 2, 8, 128), v(32, 8, 128)]
        + [v(8, 32, 128), v(8, 32, 128)]
        + [v(16, 128, 128), v(8, 16, 16, 128), v(16, 16, 128), v(16, 16, 128)]
        + [v(16, 64, 128), v(16, 64, 128), v(64, 128), v(8, 64, 128)]
        + [DMA((1,))]
        + [DMA((2,)), DMA((2,)), DMA((1,)), DMA((2,)), DMA((1,)), DMA((8,))]
        + [DMA((2,))] * 9,
        compiler_params=pltpu.CompilerParams(vmem_limit_bytes=54 << 20, collective_id=0, has_side_effects=True),
        name="whole",
    )(x[0].T, ws, w, bias.reshape(1, 128), cot)
    pair, grad, wout = pl.pallas_call(
        finish_kernel,
        out_shape=(
            jax.ShapeDtypeStruct((64, 128, 128), BF),
            jax.ShapeDtypeStruct((64, 1024), BF),
            jax.ShapeDtypeStruct((1024, 128), F32),
        ),
        in_specs=[VM, VM, VM],
        out_specs=(ANY, ANY, ANY),
        scratch_shapes=[f(1024, 128), f(1024, 128), DMA((3,))],
        compiler_params=pltpu.CompilerParams(vmem_limit_bytes=8 << 20),
        name="finish",
    )(pair, grad, wall)
    return pair, grad.T[None], wout


def solution(mesh):
    placed = (P(("row", "col"), None, None), P(), P(), P(), P("row", "col", None))
    return jax.shard_map(
        on_device,
        mesh=mesh,
        in_specs=placed,
        out_specs=(P("row", "col", None), P(("row", "col"), None, None), P()),
        check_vma=False,
    )
```

```python
import functools

import jax
import jax.numpy as jnp
from jax import lax
from jax.experimental import pallas as pl
from jax.experimental.pallas import tpu as pltpu
from jax.sharding import PartitionSpec as P

BF = jnp.bfloat16
F32 = jnp.float32
MESH = pl.DeviceIdType.MESH
NT = (((1,), (1,)), ((), ()))
DMA = pltpu.SemaphoreType.DMA


def dot(a, b):
    return jnp.dot(a, b, preferred_element_type=F32)


def dnt(a, b):
    return lax.dot_general(a, b, NT, preferred_element_type=F32)


def place():
    r, q = lax.axis_index("row"), lax.axis_index("col")
    y, zh, c = lax.div(r, 4), lax.rem(lax.div(r, 2), 2), lax.rem(r, 2)
    x, zl = lax.div(q, 2), lax.rem(q, 2)
    return r, q, y, zh, c, x, zl


def row_of(y, zh, c):
    return y * 4 + zh * 2 + c


def remote(src, dst, send, recv, to):
    return pltpu.make_async_remote_copy(
        src_ref=src, dst_ref=dst, send_sem=send, recv_sem=recv, device_id=to, device_id_type=MESH
    )


def greet(r, q):
    barrier = pltpu.get_barrier_semaphore()
    for d in range(1, 16):
        pl.semaphore_signal(barrier, inc=1, device_id=(lax.rem(r + d, 16), q), device_id_type=MESH)
    for d in range(1, 8):
        pl.semaphore_signal(barrier, inc=1, device_id=(r, lax.rem(q + d, 8)), device_id_type=MESH)


def greeted():
    pl.semaphore_wait(pltpu.get_barrier_semaphore(), 22)


def standardized(x_ref):
    x = x_ref[...].astype(F32)
    centred = x - jnp.mean(x, axis=0, keepdims=True)
    rstd = lax.rsqrt(jnp.mean(centred * centred, axis=0, keepdims=True) + 1e-5)
    return centred * rstd, rstd


def widened(ws, t):
    left = ws[:, :32]
    tiled = jnp.concatenate([left] * 4, axis=1)
    lane = lax.broadcasted_iota(jnp.int32, (64, 128), 1)
    return jnp.where(lane // 32 == t, tiled, 0.0).astype(BF)


def swapped(outer, inner):
    n = outer * inner
    to = lax.broadcasted_iota(jnp.int32, (n, n), 0)
    at = lax.broadcasted_iota(jnp.int32, (n, n), 1)
    return (at == (to % outer) * inner + to // outer).astype(F32).astype(BF)


def project(ws, xt, xs, lsend, rsend):
    right = ws.T[32:, :].astype(BF)
    for q in range(8):
        cols = xt[:, q * 128 : (q + 1) * 128]
        xs[q * 128 : (q + 1) * 128, :] = cols.T
        rsend[q] = dot(right, cols.astype(BF)).astype(BF)
    for t in range(4):
        part = xs[pl.ds(t, 256, stride=4), :].astype(BF)
        term = dot(part, widened(ws, t))
        acc = term if t == 0 else acc + term
    lsend[...] = acc.astype(BF).reshape(16, 16, 128)


def taken(ref, sem, peer):
    remote(ref, ref, sem, sem, peer).wait_recv()


def gone(ref, sem, peer):
    remote(ref, ref, sem, sem, peer).wait_send()


def to_row(p, src, dst, sems):
    r, q = p[0], p[1]
    for d in range(1, 16):
        to = lax.rem(r + d, 16)
        remote(src(to), dst.at[r], sems.at[0], sems.at[1], (to, q)).start()


def to_col(p, src, dst, sems):
    r, q = p[0], p[1]
    for d in range(1, 8):
        to = lax.rem(q + d, 8)
        remote(src(to), dst.at[q], sems.at[0], sems.at[1], (r, to)).start()


class Sends:
    def __init__(self, buf, send, recv):
        self.buf, self.send, self.recv = buf, send, recv

    def start(self, slot, to, at):
        ref = self.buf.at[:, slot]
        remote(ref, ref, self.send.at[0], self.recv.at[at], to).start()

    def arrived(self, slot, source, at):
        taken(self.buf.at[:, slot], self.recv.at[at], source)


def spread_left(p, sends):
    r, q, y, zh, c, x, zl = p
    over = x * 2 + 1 - zl
    sends.start(q, (r, over), 0)
    for d in (1, 3, 2):
        sends.start(q, (r, lax.rem(x + d, 4) * 2 + zl), 1)

    def relay():
        sends.arrived(over, (r, over), 0)
        for d in (1, 3, 2):
            sends.start(over, (r, lax.rem(x + d, 4) * 2 + zl), 1)

    def rest():
        taken(sends.buf.at[:, pl.ds(0, 6)], sends.recv.at[1], (r, over))

    def left():
        gone(sends.buf.at[:, pl.ds(0, 7)], sends.send.at[0], (r, over))

    return relay, rest, left


def spread_right(p, sends):
    r, q, y, zh, c, x, zl = p
    over = row_of(y, 1 - zh, c)
    mate = row_of(y, zh, 1 - c)
    sends.start(r, (over, q), 0)
    for d in (1, 3, 2):
        sends.start(r, (row_of(lax.rem(y + d, 4), zh, c), q), d)
    sends.start(r, (mate, q), 7)

    def relay():
        sends.arrived(over, (over, q), 0)
        for d in (1, 3, 2):
            sends.start(over, (row_of(lax.rem(y + d, 4), zh, c), q), 3 + d)
        sends.start(over, (mate, q), 7)

    def pass_on():
        for far in range(2):
            zz = zh if far == 0 else 1 - zh
            for d in (3, 1, 2):
                yd = lax.rem(y + d, 4)
                slot = row_of(yd, zz, c)
                sends.arrived(slot, (row_of(yd, zh, c), q), 3 * far + 4 - d)
                sends.start(slot, (mate, q), 7)

    def rest():
        taken(sends.buf.at[:, pl.ds(0, 8)], sends.recv.at[7], (mate, q))

    def left():
        gone(sends.buf.at[:, pl.ds(0, 15)], sends.send.at[0], (mate, q))

    return relay, pass_on, rest, left


def natural_left(l3, l4, lt):
    order = swapped(8, 16)
    for a in range(16):
        rows = dot(order, l3[a].reshape(128, 128)) * (1.0 / 128.0)
        l4[a] = rows.astype(BF)
        lt[a * 128 : (a + 1) * 128, :] = rows.T.astype(BF)


def steps(lo, hi, body):
    if hi - lo == 1:
        body(lo)
    else:
        pl.loop(lo, hi)(body)


def grad_outer(cot, wr, G, lo, hi, unroll=8):
    def body(step):
        for u in range(unroll):
            p = step * unroll + u
            o = dnt(wr[...], cot[pl.ds(2 * p, 2)].reshape(256, 128)).astype(BF)
            for h in range(2):
                G[:, pl.ds(pl.multiple_of((2 * p + h) * 32, 32), 32), :] = o[:, h * 128 : (h + 1) * 128].reshape(32, 32, 128)

    steps(lo, hi, body)


def outer_product(lt, R, O, at, m):
    for u in range(4):
        p = m * 4 + u
        o = dot(lt[...], jnp.concatenate([R[2 * p], R[2 * p + 1]], axis=1)).astype(BF)
        O[8 * at + 2 * u] = o[:, :128]
        O[8 * at + 2 * u + 1] = o[:, 128:]


def left_gradient(G, R, m, M=512):
    rows = slice(m * M, (m + 1) * M)
    for p in range(16):
        g = jnp.concatenate([G[2 * p, rows, :], G[2 * p + 1, rows, :]], axis=1)
        term = dnt(g, jnp.concatenate([R[2 * p], R[2 * p + 1]], axis=1))
        acc = term if p == 0 else acc + term
    return acc * (1.0 / 128.0)


def right_gradient(G, l4, put, lo, hi, unroll=8):
    def body(step):
        for u in range(unroll):
            p = step * unroll + u
            for k in range(8):
                rows = slice(k * 256, (k + 1) * 256)
                g = jnp.concatenate([G[2 * p, rows, :], G[2 * p + 1, rows, :]], axis=1)
                term = dot(jnp.concatenate([l4[2 * k], l4[2 * k + 1]], axis=1), g)
                acc = term if k == 0 else acc + term
            put(2 * p, acc[:, :128])
            put(2 * p + 1, acc[:, 128:])

    steps(lo, hi, body)


def weight_gradient(O, cot, at):
    for p in range(32):
        x = jnp.concatenate(
            [O[8 * at : 8 * at + 8, (2 * p + h) * 32 : (2 * p + h + 1) * 32, :].reshape(256, 128) for h in range(2)], axis=1
        )
        term = dot(x, cot[2 * p : 2 * p + 2].reshape(256, 128))
        acc = term if p == 0 else acc + term
    return acc


def of_row(O, i):
    return O[:, pl.ds(pl.multiple_of(i * 32, 32), 32), :].reshape(1024, 128)


def pair_update(O, wt, bias, out, lo, hi, unroll=8):
    wide = bias[...].astype(F32)

    def body(step):
        for u in range(unroll):
            p = step * unroll + u
            y = dot(wt[...], jnp.concatenate([of_row(O, 2 * p), of_row(O, 2 * p + 1)], axis=1))
            for h in range(2):
                out[2 * p + h] = (y[:, h * 128 : (h + 1) * 128].T + wide).astype(BF)

    steps(lo, hi, body)


def summed(buf, n):
    acc = buf[0].astype(F32)
    for k in range(1, n):
        acc = acc + buf[k].astype(F32)
    return acc


def whole_kernel(
    x, ws_ref, w, bias, cot_hbm, pair, grad, wall,
    xt, ns, xs, wf, wr, wt, cot, G, O, raw, order,
    lsend, rsend, l1, r1, l3, r3, rn, l4, lt,
    rg, rc, rcs, ry, rys, rz, r6, rin, lg, lx, l6, lin,
    wg, wgot, wsum, wc,
    cot_sem,
    la, ra, l2s, l2r, r2s, r2r, cores, ys, lxsem, zs, lo, ro, w1, w2, w3,
):
    p = place()
    r, q, y, zh, c, xx, zl = p
    mate = (row_of(y, zh, 1 - c), q)
    beside = (r, lax.rem(q + 1, 8))
    greet(r, q)
    cot_copy = pltpu.make_async_copy(cot_hbm, cot, cot_sem.at[0])
    cot_copy.start()
    ws = ws_ref[...].astype(F32)
    xhat, rstd = standardized(x)
    xt[...] = xhat
    project(ws, xt, xs, lsend, rsend)
    l1[r] = lsend[r]
    r1[q] = rsend[q]
    greeted()
    to_col(p, lambda to: rsend.at[to], r1, ra)
    to_row(p, lambda to: lsend.at[to], l1, la)
    wf[...] = w[...].astype(F32)
    for e in range(32):
        wr[e * 32 : (e + 1) * 32, :] = wf[pl.ds(e, 32, stride=32), :].astype(BF)
    chunk = [lax.rem(y + d, 4) for d in (2, 1, 3, 0)]
    for k in range(8):
        rows = pl.ds(pl.multiple_of(chunk[k // 2] * 256 + (k % 2) * 128, 128), 128)
        wt[:, k * 128 : (k + 1) * 128] = wr[rows, :].astype(F32).T.astype(BF)
    order[...] = swapped(16, 8)
    left_order, right_order = swapped(16, 16), swapped(8, 32)
    cot_copy.wait()
    grad_outer(cot, wr, G, 0, 2)
    taken(r1.at[pl.ds(0, 7)], ra.at[1], beside)
    r3[:, r] = dot(right_order, r1[...].reshape(256, 128)).reshape(32, 8, 128).astype(BF)
    rsends = Sends(r3, r2s, r2r)
    rrelay, rpass, rrest, rleft = spread_right(p, rsends)
    taken(l1.at[pl.ds(0, 15)], la.at[1], mate)
    l3[:, q] = dot(left_order, l1[...].reshape(256, 128)).astype(BF).reshape(16, 16, 128)
    lsends = Sends(l3, l2s, l2r)
    lrelay, lrest, lleft = spread_left(p, lsends)
    grad_outer(cot, wr, G, 2, 3)
    lrelay()
    rrelay()
    grad_outer(cot, wr, G, 3, 4)
    lrest()
    natural_left(l3, l4, lt)
    rpass()

    def put_right(e, v):
        rg[e] = v.reshape(8, 2, 8, 128).astype(BF)

    for half in range(2):
        right_gradient(G, l4, put_right, half, half + 1)
        es = pl.ds(half * 16, 16)
        remote(rg.at[es, :, 1 - c], rc.at[es], cores.at[0], cores.at[1], mate).start()
    rrest()
    for e in range(32):
        rn[e] = r3[e].reshape(128, 128)

    outer_product(lt, rn, O, 0, chunk[0])
    for at in range(4):
        if at < 3:
            outer_product(lt, rn, O, at + 1, chunk[at + 1])
        if at == 0:
            taken(rc, cores.at[1], mate)
            for e in range(32):
                rcs[e] = (rg[e, :, c].astype(F32) + rc[e].astype(F32)).astype(BF)
            for d in (1, 3, 2):
                to = lax.rem(y + d, 4)
                remote(rcs.at[:, pl.ds(to * 2, 2)], ry.at[d - 1], ys.at[0], ys.at[1], (row_of(to, zh, c), q)).start()
        wg[4 * at : 4 * at + 4] = weight_gradient(O, cot, at).astype(BF).reshape(4, 64, 128)
        for k in range(4 if at < 3 else 3):
            piece = k if at < 3 else lax.rem(zh * 2 + c + k + 1, 4)
            remote(wg.at[4 * at + piece], wgot.at[r], w1.at[0], w1.at[1], (chunk[at] * 4 + piece, q)).start()
    wgot[r] = wg[12 + zh * 2 + c]

    def put_left(m):
        for k in range(4 * m, 4 * m + 4):
            lg[k] = dnt(order[...], raw[k * 128 : (k + 1) * 128, :]).astype(BF)
        rows = pl.ds(m * 4, 4)
        for d in (4, 5, 3, 6, 2, 7, 1):
            to = lax.rem(q + d, 8)
            src = lg.at[rows, pl.ds(pl.multiple_of(to * 16, 16), 16), :]
            remote(src, lx.at[q, rows], lxsem.at[0], lxsem.at[1], (r, to)).start()

    for m in range(4):
        block = left_gradient(G, rn, m).astype(BF)
        if m > 0:
            put_left(m - 1)
        raw[m * 512 : (m + 1) * 512, :] = block
        if m == 2:
            taken(wgot.at[pl.ds(0, 15)], w1.at[1], mate)
            wsum[...] = summed(wgot, 16).astype(BF)
            wc[q] = wsum[...]
            to_col(p, lambda to: wsum, wc, w2)
    put_left(3)
    taken(ry, ys.at[1], mate)
    for e in range(32):
        own = rcs[e, pl.ds(y * 2, 2)].astype(F32)
        for d in range(3):
            own = own + ry[d, e].astype(F32)
        rys[e] = own.astype(BF)
    rzc = remote(rys.at[:, 1 - zh], rz, zs.at[0], zs.at[1], (row_of(y, 1 - zh, c), q))
    rzc.start()
    order2 = swapped(16, 16)

    pair_update(O, wt, bias, pair, 0, 4)

    taken(wc.at[pl.ds(0, 7)], w2.at[1], beside)
    wall[r] = summed(wc, 8).astype(BF)
    to_row(p, lambda to: wall.at[r], wall, w3)
    rzc.wait_recv()
    five = rys[:, zh].astype(F32) + rz[...].astype(F32)
    r6[...] = dot(swapped(32, 8), five.reshape(256, 128).astype(BF)).astype(BF).reshape(8, 32, 128)
    rin[q] = r6[q]
    to_col(p, lambda to: r6.at[to], rin, ro)
    taken(lx.at[pl.ds(0, 7)], lxsem.at[1], beside)
    lx[q] = lg[:, pl.ds(pl.multiple_of(q * 16, 16), 16), :]
    five = summed(lx, 8).astype(BF)
    l6[...] = dot(order2, five.reshape(256, 128)).astype(BF).reshape(16, 16, 128)
    lin[r] = l6[r]
    to_row(p, lambda to: l6.at[to], lin, lo)
    gone(rsend.at[pl.ds(0, 7)], ra.at[0], beside)
    gone(lsend.at[pl.ds(0, 15)], la.at[0], mate)
    rleft()
    lleft()
    gone(rc, cores.at[0], mate)
    gone(ry, ys.at[0], mate)
    rzc.wait_send()
    gone(wgot.at[pl.ds(0, 15)], w1.at[0], mate)
    gone(lx.at[pl.ds(0, 7)], lxsem.at[0], beside)
    gone(wc.at[pl.ds(0, 7)], w2.at[0], beside)
    gone(rin.at[pl.ds(0, 7)], ro.at[0], beside)
    taken(rin.at[pl.ds(0, 7)], ro.at[1], beside)
    right = ws[:, 32:].astype(BF)
    for k in range(8):
        ns[:, k * 128 : (k + 1) * 128] = dot(right, rin[k])
    taken(lin.at[pl.ds(0, 15)], lo.at[1], mate)
    flat = lin[...].reshape(256, 128)
    for t in range(4):
        xs[pl.ds(t, 256, stride=4), :] = dnt(flat, widened(ws, t))
    for k in range(8):
        cols = slice(k * 128, (k + 1) * 128)
        ng = ns[:, cols] + xs[cols, :].T
        xh = xt[:, cols]
        first = jnp.mean(ng, axis=0, keepdims=True)
        second = jnp.mean(ng * xh, axis=0, keepdims=True)
        grad[:, cols] = (rstd[:, cols] * (ng - first - xh * second)).astype(BF)
    taken(wall.at[pl.ds(0, 15)], w3.at[1], mate)
    gone(lin.at[pl.ds(0, 15)], lo.at[0], mate)
    gone(wall.at[pl.ds(0, 15)], w3.at[0], mate)


def finish_kernel(pair, grad, wall, pair_out, grad_out, wout, wf, wo, sems):
    cps = [
        pltpu.make_async_copy(pair, pair_out, sems.at[0]),
        pltpu.make_async_copy(grad, grad_out, sems.at[1]),
        pltpu.make_async_copy(wo, wout, sems.at[2]),
    ]
    cps[0].start()
    cps[1].start()
    for k in range(16):
        wf[k * 64 : (k + 1) * 64, :] = wall[k].astype(F32)
    for k in range(32):
        wo[k * 32 : (k + 1) * 32, :] = wf[pl.ds(k, 32, stride=32), :]
    cps[2].start()
    for cp in cps:
        cp.wait()


VM = pl.BlockSpec(memory_space=pltpu.VMEM)
ANY = pl.BlockSpec(memory_space=pl.ANY)


def on_device(x, ws, w, bias, cot):
    v = lambda *s: pltpu.VMEM(s, BF)
    f = lambda *s: pltpu.VMEM(s, F32)
    pair, grad, wall = pl.pallas_call(
        whole_kernel,
        out_shape=(v(64, 128, 128), v(64, 1024), v(16, 64, 128)),
        in_specs=[VM, VM, VM, VM, ANY],
        out_specs=(VM, VM, VM),
        scratch_shapes=[f(64, 1024), f(64, 1024), f(1024, 64), f(1024, 128), v(1024, 128), v(128, 1024), v(64, 128, 128)]
        + [v(32, 2048, 128), v(32, 2048, 128), v(2048, 128), v(128, 128)]
        + [v(16, 16, 128), v(8, 32, 128), v(16, 16, 128), v(8, 32, 128), v(16, 8, 16, 128), v(32, 16, 8, 128), v(32, 128, 128)]
        + [v(16, 128, 128), v(2048, 128)]
        + [v(32, 8, 2, 8, 128), v(32, 8, 8, 128), v(32, 8, 8, 128), v(3, 32, 2, 8, 128), v(32, 2, 8, 128), v(32, 8, 128)]
        + [v(8, 32, 128), v(8, 32, 128)]
        + [v(16, 128, 128), v(8, 16, 16, 128), v(16, 16, 128), v(16, 16, 128)]
        + [v(16, 64, 128), v(16, 64, 128), v(64, 128), v(8, 64, 128)]
        + [DMA((1,))]
        + [DMA((2,)), DMA((2,)), DMA((1,)), DMA((2,)), DMA((1,)), DMA((8,))]
        + [DMA((2,))] * 9,
        compiler_params=pltpu.CompilerParams(vmem_limit_bytes=54 << 20, collective_id=0, has_side_effects=True),
        name="whole",
    )(x[0].T, ws, w, bias.reshape(1, 128), cot)
    pair, grad, wout = pl.pallas_call(
        finish_kernel,
        out_shape=(
            jax.ShapeDtypeStruct((64, 128, 128), BF),
            jax.ShapeDtypeStruct((64, 1024), BF),
            jax.ShapeDtypeStruct((1024, 128), F32),
        ),
        in_specs=[VM, VM, VM],
        out_specs=(ANY, ANY, ANY),
        scratch_shapes=[f(1024, 128), f(1024, 128), DMA((3,))],
        compiler_params=pltpu.CompilerParams(vmem_limit_bytes=8 << 20),
        name="finish",
    )(pair, grad, wall)
    return pair, grad.T[None], wout


def solution(mesh):
    placed = (P(("row", "col"), None, None), P(), P(), P(), P("row", "col", None))
    return jax.shard_map(
        on_device,
        mesh=mesh,
        in_specs=placed,
        out_specs=(P("row", "col", None), P(("row", "col"), None, None), P()),
        check_vma=False,
    )
```

```python
import functools

import jax
import jax.numpy as jnp
from jax import lax
from jax.experimental import pallas as pl
from jax.experimental.pallas import tpu as pltpu
from jax.sharding import PartitionSpec as P

BF = jnp.bfloat16
F32 = jnp.float32
MESH = pl.DeviceIdType.MESH
NT = (((1,), (1,)), ((), ()))
DMA = pltpu.SemaphoreType.DMA


def dot(a, b):
    return jnp.dot(a, b, preferred_element_type=F32)


def dnt(a, b):
    return lax.dot_general(a, b, NT, preferred_element_type=F32)


def place():
    r, q = lax.axis_index("row"), lax.axis_index("col")
    y, zh, c = lax.div(r, 4), lax.rem(lax.div(r, 2), 2), lax.rem(r, 2)
    x, zl = lax.div(q, 2), lax.rem(q, 2)
    return r, q, y, zh, c, x, zl


def row_of(y, zh, c):
    return y * 4 + zh * 2 + c


def remote(src, dst, send, recv, to):
    return pltpu.make_async_remote_copy(
        src_ref=src, dst_ref=dst, send_sem=send, recv_sem=recv, device_id=to, device_id_type=MESH
    )


def greet(r, q):
    barrier = pltpu.get_barrier_semaphore()
    for d in range(1, 16):
        pl.semaphore_signal(barrier, inc=1, device_id=(lax.rem(r + d, 16), q), device_id_type=MESH)
    for d in range(1, 8):
        pl.semaphore_signal(barrier, inc=1, device_id=(r, lax.rem(q + d, 8)), device_id_type=MESH)


def greeted():
    pl.semaphore_wait(pltpu.get_barrier_semaphore(), 22)


def standardized(x_ref):
    x = x_ref[...].astype(F32)
    centred = x - jnp.mean(x, axis=0, keepdims=True)
    rstd = lax.rsqrt(jnp.mean(centred * centred, axis=0, keepdims=True) + 1e-5)
    return centred * rstd, rstd


def widened(ws, t):
    left = ws[:, :32]
    tiled = jnp.concatenate([left] * 4, axis=1)
    lane = lax.broadcasted_iota(jnp.int32, (64, 128), 1)
    return jnp.where(lane // 32 == t, tiled, 0.0).astype(BF)


def swapped(outer, inner):
    n = outer * inner
    to = lax.broadcasted_iota(jnp.int32, (n, n), 0)
    at = lax.broadcasted_iota(jnp.int32, (n, n), 1)
    return (at == (to % outer) * inner + to // outer).astype(F32).astype(BF)


def project(ws, xt, xs, lsend, rsend):
    right = ws.T[32:, :].astype(BF)
    for q in range(8):
        cols = xt[:, q * 128 : (q + 1) * 128]
        xs[q * 128 : (q + 1) * 128, :] = cols.T
        rsend[q] = dot(right, cols.astype(BF)).astype(BF)
    for t in range(4):
        part = xs[pl.ds(t, 256, stride=4), :].astype(BF)
        term = dot(part, widened(ws, t))
        acc = term if t == 0 else acc + term
    lsend[...] = acc.astype(BF).reshape(16, 16, 128)


def taken(ref, sem, peer):
    remote(ref, ref, sem, sem, peer).wait_recv()


def gone(ref, sem, peer):
    remote(ref, ref, sem, sem, peer).wait_send()


def to_row(p, src, dst, sems):
    r, q = p[0], p[1]
    for d in range(1, 16):
        to = lax.rem(r + d, 16)
        remote(src(to), dst.at[r], sems.at[0], sems.at[1], (to, q)).start()


def to_col(p, src, dst, sems):
    r, q = p[0], p[1]
    for d in range(1, 8):
        to = lax.rem(q + d, 8)
        remote(src(to), dst.at[q], sems.at[0], sems.at[1], (r, to)).start()


class Sends:
    def __init__(self, buf, send, recv):
        self.buf, self.send, self.recv = buf, send, recv

    def start(self, slot, to, at):
        ref = self.buf.at[:, slot]
        remote(ref, ref, self.send.at[0], self.recv.at[at], to).start()

    def arrived(self, slot, source, at):
        taken(self.buf.at[:, slot], self.recv.at[at], source)


def spread_left(p, sends):
    r, q, y, zh, c, x, zl = p
    over = x * 2 + 1 - zl
    sends.start(q, (r, over), 0)
    for d in (1, 3, 2):
        sends.start(q, (r, lax.rem(x + d, 4) * 2 + zl), 1)

    def relay():
        sends.arrived(over, (r, over), 0)
        for d in (1, 3, 2):
            sends.start(over, (r, lax.rem(x + d, 4) * 2 + zl), 1)

    def rest():
        taken(sends.buf.at[:, pl.ds(0, 6)], sends.recv.at[1], (r, over))

    def left():
        gone(sends.buf.at[:, pl.ds(0, 7)], sends.send.at[0], (r, over))

    return relay, rest, left


def spread_right(p, sends):
    r, q, y, zh, c, x, zl = p
    over = row_of(y, 1 - zh, c)
    mate = row_of(y, zh, 1 - c)
    sends.start(r, (over, q), 0)
    for d in (1, 3, 2):
        sends.start(r, (row_of(lax.rem(y + d, 4), zh, c), q), d)
    sends.start(r, (mate, q), 7)

    def relay():
        sends.arrived(over, (over, q), 0)
        for d in (1, 3, 2):
            sends.start(over, (row_of(lax.rem(y + d, 4), zh, c), q), 3 + d)
        sends.start(over, (mate, q), 7)

    def pass_on():
        for far in range(2):
            zz = zh if far == 0 else 1 - zh
            for d in (3, 1, 2):
                yd = lax.rem(y + d, 4)
                slot = row_of(yd, zz, c)
                sends.arrived(slot, (row_of(yd, zh, c), q), 3 * far + 4 - d)
                sends.start(slot, (mate, q), 7)

    def rest():
        taken(sends.buf.at[:, pl.ds(0, 8)], sends.recv.at[7], (mate, q))

    def left():
        gone(sends.buf.at[:, pl.ds(0, 15)], sends.send.at[0], (mate, q))

    return relay, pass_on, rest, left


def natural_left(l3, l4, lt):
    order = swapped(8, 16)
    for a in range(16):
        rows = dot(order, l3[a].reshape(128, 128)) * (1.0 / 128.0)
        l4[a] = rows.astype(BF)
        lt[a * 128 : (a + 1) * 128, :] = rows.T.astype(BF)


def steps(lo, hi, body):
    if hi - lo == 1:
        body(lo)
    else:
        pl.loop(lo, hi)(body)


def grad_outer(cot, wr, G, lo, hi, unroll=8):
    def body(step):
        for u in range(unroll):
            p = step * unroll + u
            o = dnt(wr[...], cot[pl.ds(2 * p, 2)].reshape(256, 128)).astype(BF)
            for h in range(2):
                G[:, pl.ds(pl.multiple_of((2 * p + h) * 32, 32), 32), :] = o[:, h * 128 : (h + 1) * 128].reshape(32, 32, 128)

    steps(lo, hi, body)


def outer_product(lt, R, O, at, m):
    for u in range(4):
        p = m * 4 + u
        o = dot(lt[...], jnp.concatenate([R[2 * p], R[2 * p + 1]], axis=1)).astype(BF)
        O[8 * at + 2 * u] = o[:, :128]
        O[8 * at + 2 * u + 1] = o[:, 128:]


def left_gradient(G, R, m, M=512):
    rows = slice(m * M, (m + 1) * M)
    for p in range(16):
        g = jnp.concatenate([G[2 * p, rows, :], G[2 * p + 1, rows, :]], axis=1)
        term = dnt(g, jnp.concatenate([R[2 * p], R[2 * p + 1]], axis=1))
        acc = term if p == 0 else acc + term
    return acc * (1.0 / 128.0)


def right_gradient(G, l4, put, lo, hi, unroll=8):
    def body(step):
        for u in range(unroll):
            p = step * unroll + u
            for k in range(8):
                rows = slice(k * 256, (k + 1) * 256)
                g = jnp.concatenate([G[2 * p, rows, :], G[2 * p + 1, rows, :]], axis=1)
                term = dot(jnp.concatenate([l4[2 * k], l4[2 * k + 1]], axis=1), g)
                acc = term if k == 0 else acc + term
            put(2 * p, acc[:, :128])
            put(2 * p + 1, acc[:, 128:])

    steps(lo, hi, body)


def weight_gradient(O, cot, at):
    for p in range(32):
        x = jnp.concatenate(
            [O[8 * at : 8 * at + 8, (2 * p + h) * 32 : (2 * p + h + 1) * 32, :].reshape(256, 128) for h in range(2)], axis=1
        )
        term = dot(x, cot[2 * p : 2 * p + 2].reshape(256, 128))
        acc = term if p == 0 else acc + term
    return acc


def of_row(O, i):
    return O[:, pl.ds(pl.multiple_of(i * 32, 32), 32), :].reshape(1024, 128)


def pair_update(O, wt, bias, out, lo, hi, unroll=8):
    wide = bias[...].astype(F32)

    def body(step):
        for u in range(unroll):
            p = step * unroll + u
            y = dot(wt[...], jnp.concatenate([of_row(O, 2 * p), of_row(O, 2 * p + 1)], axis=1))
            for h in range(2):
                out[2 * p + h] = (y[:, h * 128 : (h + 1) * 128].T + wide).astype(BF)

    steps(lo, hi, body)


def summed(buf, n):
    acc = buf[0].astype(F32)
    for k in range(1, n):
        acc = acc + buf[k].astype(F32)
    return acc


def whole_kernel(
    x, ws_ref, w, bias, cot_hbm, pair, grad, wall,
    xt, ns, xs, wf, wr, wt, cot, G, O, raw, order,
    lsend, rsend, l1, r1, l3, r3, rn, l4, lt,
    rg, rc, rcs, ry, rys, rz, r6, rin, lg, lx, l6, lin,
    wg, wgot, wsum, wc,
    cot_sem,
    la, ra, l2s, l2r, r2s, r2r, cores, ys, lxsem, zs, lo, ro, w1, w2, w3,
):
    p = place()
    r, q, y, zh, c, xx, zl = p
    mate = (row_of(y, zh, 1 - c), q)
    beside = (r, lax.rem(q + 1, 8))
    greet(r, q)
    cot_copy = pltpu.make_async_copy(cot_hbm, cot, cot_sem.at[0])
    cot_copy.start()
    ws = ws_ref[...].astype(F32)
    xhat, rstd = standardized(x)
    xt[...] = xhat
    project(ws, xt, xs, lsend, rsend)
    l1[r] = lsend[r]
    r1[q] = rsend[q]
    greeted()
    to_col(p, lambda to: rsend.at[to], r1, ra)
    to_row(p, lambda to: lsend.at[to], l1, la)
    wf[...] = w[...].astype(F32)
    for e in range(32):
        wr[e * 32 : (e + 1) * 32, :] = wf[pl.ds(e, 32, stride=32), :].astype(BF)
    chunk = [lax.rem(y + d, 4) for d in (2, 1, 3, 0)]
    for k in range(8):
        rows = pl.ds(pl.multiple_of(chunk[k // 2] * 256 + (k % 2) * 128, 128), 128)
        wt[:, k * 128 : (k + 1) * 128] = wr[rows, :].astype(F32).T.astype(BF)
    order[...] = swapped(16, 8)
    left_order, right_order = swapped(16, 16), swapped(8, 32)
    cot_copy.wait()
    grad_outer(cot, wr, G, 0, 2)
    taken(r1.at[pl.ds(0, 7)], ra.at[1], beside)
    r3[:, r] = dot(right_order, r1[...].reshape(256, 128)).reshape(32, 8, 128).astype(BF)
    rsends = Sends(r3, r2s, r2r)
    rrelay, rpass, rrest, rleft = spread_right(p, rsends)
    taken(l1.at[pl.ds(0, 15)], la.at[1], mate)
    l3[:, q] = dot(left_order, l1[...].reshape(256, 128)).astype(BF).reshape(16, 16, 128)
    lsends = Sends(l3, l2s, l2r)
    lrelay, lrest, lleft = spread_left(p, lsends)
    grad_outer(cot, wr, G, 2, 3)
    lrelay()
    rrelay()
    grad_outer(cot, wr, G, 3, 4)
    lrest()
    natural_left(l3, l4, lt)
    rpass()

    def put_right(e, v):
        rg[e] = v.reshape(8, 2, 8, 128).astype(BF)

    for half in range(2):
        right_gradient(G, l4, put_right, half, half + 1)
        es = pl.ds(half * 16, 16)
        remote(rg.at[es, :, 1 - c], rc.at[es], cores.at[0], cores.at[1], mate).start()
    rrest()
    for e in range(32):
        rn[e] = r3[e].reshape(128, 128)

    outer_product(lt, rn, O, 0, chunk[0])
    for at in range(4):
        if at < 3:
            outer_product(lt, rn, O, at + 1, chunk[at + 1])
        if at == 0:
            taken(rc, cores.at[1], mate)
            for e in range(32):
                rcs[e] = (rg[e, :, c].astype(F32) + rc[e].astype(F32)).astype(BF)
            for d in (1, 3, 2):
                to = lax.rem(y + d, 4)
                remote(rcs.at[:, pl.ds(to * 2, 2)], ry.at[d - 1], ys.at[0], ys.at[1], (row_of(to, zh, c), q)).start()
        wg[4 * at : 4 * at + 4] = weight_gradient(O, cot, at).astype(BF).reshape(4, 64, 128)
        for k in range(4 if at < 3 else 3):
            piece = k if at < 3 else lax.rem(zh * 2 + c + k + 1, 4)
            remote(wg.at[4 * at + piece], wgot.at[r], w1.at[0], w1.at[1], (chunk[at] * 4 + piece, q)).start()
    wgot[r] = wg[12 + zh * 2 + c]

    def put_left(m):
        for k in range(4 * m, 4 * m + 4):
            lg[k] = dnt(order[...], raw[k * 128 : (k + 1) * 128, :]).astype(BF)
        rows = pl.ds(m * 4, 4)
        for d in (4, 5, 3, 6, 2, 7, 1):
            to = lax.rem(q + d, 8)
            src = lg.at[rows, pl.ds(pl.multiple_of(to * 16, 16), 16), :]
            remote(src, lx.at[q, rows], lxsem.at[0], lxsem.at[1], (r, to)).start()

    for m in range(4):
        block = left_gradient(G, rn, m).astype(BF)
        if m > 0:
            put_left(m - 1)
        raw[m * 512 : (m + 1) * 512, :] = block
        if m == 0:
            taken(ry, ys.at[1], mate)
            for e in range(32):
                own = rcs[e, pl.ds(y * 2, 2)].astype(F32)
                for d in range(3):
                    own = own + ry[d, e].astype(F32)
                rys[e] = own.astype(BF)
            rzc = remote(rys.at[:, 1 - zh], rz, zs.at[0], zs.at[1], (row_of(y, 1 - zh, c), q))
            rzc.start()
        if m == 2:
            taken(wgot.at[pl.ds(0, 15)], w1.at[1], mate)
            wsum[...] = summed(wgot, 16).astype(BF)
            wc[q] = wsum[...]
            to_col(p, lambda to: wsum, wc, w2)
    put_left(3)
    rzc.wait_recv()
    five = rys[:, zh].astype(F32) + rz[...].astype(F32)
    r6[...] = dot(swapped(32, 8), five.reshape(256, 128).astype(BF)).astype(BF).reshape(8, 32, 128)
    rin[q] = r6[q]
    to_col(p, lambda to: r6.at[to], rin, ro)
    order2 = swapped(16, 16)

    pair_update(O, wt, bias, pair, 0, 4)

    taken(wc.at[pl.ds(0, 7)], w2.at[1], beside)
    wall[r] = summed(wc, 8).astype(BF)
    to_row(p, lambda to: wall.at[r], wall, w3)
    taken(lx.at[pl.ds(0, 7)], lxsem.at[1], beside)
    lx[q] = lg[:, pl.ds(pl.multiple_of(q * 16, 16), 16), :]
    five = summed(lx, 8).astype(BF)
    l6[...] = dot(order2, five.reshape(256, 128)).astype(BF).reshape(16, 16, 128)
    lin[r] = l6[r]
    to_row(p, lambda to: l6.at[to], lin, lo)
    gone(rsend.at[pl.ds(0, 7)], ra.at[0], beside)
    gone(lsend.at[pl.ds(0, 15)], la.at[0], mate)
    rleft()
    lleft()
    gone(rc, cores.at[0], mate)
    gone(ry, ys.at[0], mate)
    rzc.wait_send()
    gone(wgot.at[pl.ds(0, 15)], w1.at[0], mate)
    gone(lx.at[pl.ds(0, 7)], lxsem.at[0], beside)
    gone(wc.at[pl.ds(0, 7)], w2.at[0], beside)
    gone(rin.at[pl.ds(0, 7)], ro.at[0], beside)
    taken(rin.at[pl.ds(0, 7)], ro.at[1], beside)
    right = ws[:, 32:].astype(BF)
    for k in range(8):
        ns[:, k * 128 : (k + 1) * 128] = dot(right, rin[k])
    taken(lin.at[pl.ds(0, 15)], lo.at[1], mate)
    flat = lin[...].reshape(256, 128)
    for t in range(4):
        xs[pl.ds(t, 256, stride=4), :] = dnt(flat, widened(ws, t))
    for k in range(8):
        cols = slice(k * 128, (k + 1) * 128)
        ng = ns[:, cols] + xs[cols, :].T
        xh = xt[:, cols]
        first = jnp.mean(ng, axis=0, keepdims=True)
        second = jnp.mean(ng * xh, axis=0, keepdims=True)
        grad[:, cols] = (rstd[:, cols] * (ng - first - xh * second)).astype(BF)
    taken(wall.at[pl.ds(0, 15)], w3.at[1], mate)
    gone(lin.at[pl.ds(0, 15)], lo.at[0], mate)
    gone(wall.at[pl.ds(0, 15)], w3.at[0], mate)


def finish_kernel(pair, grad, wall, pair_out, grad_out, wout, wf, wo, sems):
    cps = [
        pltpu.make_async_copy(pair, pair_out, sems.at[0]),
        pltpu.make_async_copy(grad, grad_out, sems.at[1]),
        pltpu.make_async_copy(wo, wout, sems.at[2]),
    ]
    cps[0].start()
    cps[1].start()
    for k in range(16):
        wf[k * 64 : (k + 1) * 64, :] = wall[k].astype(F32)
    for k in range(32):
        wo[k * 32 : (k + 1) * 32, :] = wf[pl.ds(k, 32, stride=32), :]
    cps[2].start()
    for cp in cps:
        cp.wait()


VM = pl.BlockSpec(memory_space=pltpu.VMEM)
ANY = pl.BlockSpec(memory_space=pl.ANY)


def on_device(x, ws, w, bias, cot):
    v = lambda *s: pltpu.VMEM(s, BF)
    f = lambda *s: pltpu.VMEM(s, F32)
    pair, grad, wall = pl.pallas_call(
        whole_kernel,
        out_shape=(v(64, 128, 128), v(64, 1024), v(16, 64, 128)),
        in_specs=[VM, VM, VM, VM, ANY],
        out_specs=(VM, VM, VM),
        scratch_shapes=[f(64, 1024), f(64, 1024), f(1024, 64), f(1024, 128), v(1024, 128), v(128, 1024), v(64, 128, 128)]
        + [v(32, 2048, 128), v(32, 2048, 128), v(2048, 128), v(128, 128)]
        + [v(16, 16, 128), v(8, 32, 128), v(16, 16, 128), v(8, 32, 128), v(16, 8, 16, 128), v(32, 16, 8, 128), v(32, 128, 128)]
        + [v(16, 128, 128), v(2048, 128)]
        + [v(32, 8, 2, 8, 128), v(32, 8, 8, 128), v(32, 8, 8, 128), v(3, 32, 2, 8, 128), v(32, 2, 8, 128), v(32, 8, 128)]
        + [v(8, 32, 128), v(8, 32, 128)]
        + [v(16, 128, 128), v(8, 16, 16, 128), v(16, 16, 128), v(16, 16, 128)]
        + [v(16, 64, 128), v(16, 64, 128), v(64, 128), v(8, 64, 128)]
        + [DMA((1,))]
        + [DMA((2,)), DMA((2,)), DMA((1,)), DMA((2,)), DMA((1,)), DMA((8,))]
        + [DMA((2,))] * 9,
        compiler_params=pltpu.CompilerParams(vmem_limit_bytes=54 << 20, collective_id=0, has_side_effects=True),
        name="whole",
    )(x[0].T, ws, w, bias.reshape(1, 128), cot)
    pair, grad, wout = pl.pallas_call(
        finish_kernel,
        out_shape=(
            jax.ShapeDtypeStruct((64, 128, 128), BF),
            jax.ShapeDtypeStruct((64, 1024), BF),
            jax.ShapeDtypeStruct((1024, 128), F32),
        ),
        in_specs=[VM, VM, VM],
        out_specs=(ANY, ANY, ANY),
        scratch_shapes=[f(1024, 128), f(1024, 128), DMA((3,))],
        compiler_params=pltpu.CompilerParams(vmem_limit_bytes=8 << 20),
        name="finish",
    )(pair, grad, wall)
    return pair, grad.T[None], wout


def solution(mesh):
    placed = (P(("row", "col"), None, None), P(), P(), P(), P("row", "col", None))
    return jax.shard_map(
        on_device,
        mesh=mesh,
        in_specs=placed,
        out_specs=(P("row", "col", None), P(("row", "col"), None, None), P()),
        check_vma=False,
    )
```
